256 devices in a mesh: seg: 64 (over z, x, core), bin: 4 (over y).
Axes of the slice: x: 4, y: 4, z: 8, core: 2. Of those that a mesh axis runs over, the one named last changes fastest.
Arguments:
- magnet_real: bfloat16 [512, 8, 32768], P('seg', None, 'bin'), may hold values from -8 to 8
- magnet_imag: bfloat16 [512, 8, 32768], P('seg', None, 'bin'), may hold values from -8 to 8
- detector_real: bfloat16 [512, 2, 32768], P('seg', None, 'bin'), may hold values from -8 to 8
- detector_imag: bfloat16 [512, 2, 32768], P('seg', None, 'bin'), may hold values from -8 to 8
- valid: int32 [512], P('seg'), may hold values 0 or 1
- intersection: float32 [32768], P('bin'), may hold values from 0.1 to 1
Outputs:
- cleaned_real: float32 [512, 32768], P('seg', 'bin')
- cleaned_imag: float32 [512, 32768], P('seg', 'bin')
- estimate: float32 [512], P('seg')
The draws below stay inside these ranges and needn't reach their ends.
Inputs may be any that keep to these rules, and one draw needn't show every extreme that they name: `valid`: 1 keeps a segment in the spectral sums, 0 vetoes it.
All inputs are finite; a program needn't handle non-finite values. No bound on the sum of `valid` on one device may be relied on, other than what follows from the above.
Results may differ from the reference program's by a relative error of at most 0.0005.
Values sent between devices are 32-bit elements; how exact they have to be, the bound alone decides.
No kernel may reach another device: no remote copies, remote signals or barrier semaphores. Data moves between devices by JAX's collectives and lax.ppermute only.
A program may use at most 64 MiB of HBM per device.

```python
import math
import jax
import jax.numpy as jnp
from jax import lax

CHANNELS = 8
DETECTORS = 2
BINS = 32768
SEGS = 512


def schumann_sources(key):
    base = jax.random.fold_in(key, 9173)
    first, second = jax.random.split(base, 2)
    shape = (SEGS, 3, BINS)
    spread = 0.70710677
    src_real = jax.random.normal(first, shape, jnp.float32) * spread
    src_imag = jax.random.normal(second, shape, jnp.float32) * spread
    return (src_real, src_imag)


def complex_mixing(key, salt, rows):
    base = jax.random.fold_in(key, salt)
    first, second = jax.random.split(base, 2)
    spread = 0.57735027
    mix_real = jax.random.normal(first, (rows, 3, BINS), jnp.float32) * spread
    mix_imag = jax.random.normal(second, (rows, 3, BINS), jnp.float32) * spread
    return (mix_real, mix_imag)


def mixed_part(key, salt, rows, noise_scale, component):
    src_real, src_imag = schumann_sources(key)
    mix_real, mix_imag = complex_mixing(key, salt, rows)
    total = jnp.zeros((SEGS, rows, BINS), jnp.float32)
    for source in range(3):
        field_real = src_real[:, None, source, :]
        field_imag = src_imag[:, None, source, :]
        coeff_real = mix_real[None, :, source, :]
        coeff_imag = mix_imag[None, :, source, :]
        if component == 1:
            total = total + coeff_real * field_imag + coeff_imag * field_real
        else:
            total = total + coeff_real * field_real - coeff_imag * field_imag
    noise_key = jax.random.fold_in(key, salt + 1 + component)
    noise = jax.random.normal(noise_key, (SEGS, rows, BINS), jnp.float32) * noise_scale
    return total + noise


def magnet_component(key, component):
    values = mixed_part(key, 101, CHANNELS, 0.6, component)
    return jnp.clip(values, -8.0, 8.0).astype(jnp.bfloat16)


def detector_component(key, component):
    values = mixed_part(key, 211, DETECTORS, 0.7, component)
    return jnp.clip(values, -8.0, 8.0).astype(jnp.bfloat16)


def draw_magnet_real(key, part):
    return magnet_component(key, 0)


def draw_magnet_imag(key, part):
    return magnet_component(key, 1)


def draw_detector_real(key, part):
    return detector_component(key, 0)


def draw_detector_imag(key, part):
    return detector_component(key, 1)


def touch_ends(values, key, smallest, largest):
    longest = values.shape.index(max(values.shape))
    spots = []
    for shift in (0, 1):
        where = [jax.random.randint(jax.random.fold_in(key, axis), (), 0, length) for axis, length in enumerate(values.shape)]
        where[longest] = (where[longest] + shift) % values.shape[longest]
        spots.append(tuple(where))
    return values.at[spots[0]].set(smallest).at[spots[1]].set(largest)


def shard_levels(own_key, dims, cuts, least, top_value):
    loudness, own = 1.0, jax.random.fold_in(own_key, 6)
    for dim, parts in cuts:
        heights = jnp.exp(jax.random.uniform(jax.random.fold_in(own, dim), (parts,), jnp.float32, least / len(cuts), top_value / len(cuts)))
        loudness = loudness * jnp.repeat(heights, dims[dim] // parts).reshape([-1 if axis == dim else 1 for axis in range(len(dims))])
    return loudness


def setup_inputs(seed: int = 0) -> dict:
    seeds = jax.random.split(jax.random.key(seed), 7)
    return {
        "magnet_real": draw_magnet_real(jax.random.fold_in(seeds[6], 71), 0),
        "magnet_imag": draw_magnet_imag(jax.random.fold_in(seeds[6], 71), 0),
        "detector_real": draw_detector_real(jax.random.fold_in(seeds[6], 71), 0),
        "detector_imag": draw_detector_imag(jax.random.fold_in(seeds[6], 71), 0),
        "valid": touch_ends((jax.random.randint(seeds[4], (SEGS,), 0, 4) < 3).astype(jnp.int32), jax.random.fold_in(seeds[4], 1), 0, 1),
        "intersection": jnp.clip(jnp.exp(math.log(1.0) - 2.3025851 * jax.random.uniform(seeds[5], (BINS,), jnp.float32) ** shard_levels(seeds[5], (BINS,), ((0, 4),), -0.2, 0.2)), 0.1, 1.0),
    }


def wiener_solve(s_real, s_imag, p_real, p_imag):
    channels = s_real.shape[0]
    matrix_size = 2 * channels

    def matrix_entry(i, j):
        if i < channels and j < channels:
            value = s_real[i, j]
        elif i < channels:
            value = -s_imag[i, j - channels]
        elif j < channels:
            value = s_imag[i - channels, j]
        else:
            value = s_real[i - channels, j - channels]
        if i == j:
            value = value + 1.0
        return value

    def right_entry(i):
        if i < channels:
            return p_real[i]
        return p_imag[i - channels]
    factor = [[None] * matrix_size for i in range(matrix_size)]
    for j in range(matrix_size):
        running = matrix_entry(j, j)
        for k in range(j):
            running = running - factor[j][k] * factor[j][k]
        factor[j][j] = jnp.sqrt(running)
        inverse = 1.0 / factor[j][j]
        for i in range(j + 1, matrix_size):
            running = matrix_entry(i, j)
            for k in range(j):
                running = running - factor[i][k] * factor[j][k]
            factor[i][j] = running * inverse
    forward = []
    for i in range(matrix_size):
        running = right_entry(i)
        for k in range(i):
            running = running - factor[i][k] * forward[k]
        forward.append(running / factor[i][i])
    backward = [None] * matrix_size
    for i in reversed(range(matrix_size)):
        running = forward[i]
        for k in range(i + 1, matrix_size):
            running = running - factor[k][i] * backward[k]
        backward[i] = running / factor[i][i]
    return (jnp.stack(backward[:channels]), jnp.stack(backward[channels:]))

def reference(magnet_real, magnet_imag, detector_real, detector_imag, valid, intersection):
    block_bins = math.gcd(BINS, 1024)
    block_count = BINS // block_bins
    keep = valid.astype(jnp.float32)[:, None, None]

    def contract(left, right):
        return jnp.einsum('scf,sdf->cdf', left, right, precision=lax.Precision.HIGHEST)

    def project(filt, field):
        return jnp.einsum('ckf,scf->skf', filt, field, precision=lax.Precision.HIGHEST)

    def block_work(start):
        field_real = lax.dynamic_slice_in_dim(magnet_real, start, block_bins, 2).astype(jnp.float32)
        field_imag = lax.dynamic_slice_in_dim(magnet_imag, start, block_bins, 2).astype(jnp.float32)
        strain_real = lax.dynamic_slice_in_dim(detector_real, start, block_bins, 2).astype(jnp.float32)
        strain_imag = lax.dynamic_slice_in_dim(detector_imag, start, block_bins, 2).astype(jnp.float32)
        kept_real = field_real * keep
        kept_imag = field_imag * keep
        s_real = contract(kept_real, field_real) + contract(kept_imag, field_imag)
        s_imag = contract(kept_imag, field_real) - contract(kept_real, field_imag)
        p_real = contract(kept_real, strain_real) + contract(kept_imag, strain_imag)
        p_imag = contract(kept_imag, strain_real) - contract(kept_real, strain_imag)
        filt_real, filt_imag = wiener_solve(s_real, s_imag, p_real, p_imag)
        clean_real = strain_real - project(filt_real, field_real) - project(filt_imag, field_imag)
        clean_imag = strain_imag - project(filt_real, field_imag) + project(filt_imag, field_real)
        cross_real = clean_real[:, 0] * clean_real[:, 1] + clean_imag[:, 0] * clean_imag[:, 1]
        cross_imag = clean_imag[:, 0] * clean_real[:, 1] - clean_real[:, 0] * clean_imag[:, 1]
        return (cross_real, cross_imag)
    block_starts = jnp.arange(block_count, dtype=jnp.int32) * block_bins
    real_blocks, imag_blocks = lax.map(block_work, block_starts)
    cleaned_real = jnp.moveaxis(real_blocks, 0, 1).reshape(SEGS, BINS)
    cleaned_imag = jnp.moveaxis(imag_blocks, 0, 1).reshape(SEGS, BINS)
    summed = jnp.dot(cleaned_real, intersection, precision=lax.Precision.HIGHEST)
    estimate = summed / jnp.sqrt(jnp.sum(intersection * intersection))
    return (cleaned_real, cleaned_imag, estimate)
```

```python
import jax
import jax.numpy as jnp
from jax import lax
from jax.experimental import pallas as pl
from jax.experimental.pallas import tpu as pltpu
from jax.sharding import Mesh
from jax.sharding import PartitionSpec as P


SEG = ("z", "x", "c")
LANES = 128
CH = 8
DET = 2
ROWS = 96
WROWS = 32
VMEM = pltpu.VMEM
SMEM = pltpu.SMEM
F32 = jnp.float32


def gray(i):
    return i ^ (i >> 1)


def flip_pairs(size, shift, bit):
    where = {gray((i - shift) % size): i for i in range(size)}
    return [(i, where[gray((i - shift) % size) ^ (1 << bit)]) for i in range(size)]


STEPS = (
    (("x", 0, 0), ("x", 0, 1), ("z", 0, 0), ("z", 0, 1), ("z", 0, 2)),
    (("x", 0, 1), ("x", 0, 0), ("z", 1, 0), ("z", 1, 2), ("z", 1, 1)),
)
SUB = 2


def swap_step(value, at, sizes):
    nz, nx, nc = sizes["z"], sizes["x"], sizes["c"]
    pairs = []
    for z in range(nz):
        for x in range(nx):
            for c in range(nc):
                axis, shift, bit = STEPS[c][at]
                where = {"z": z, "x": x}
                where[axis] = dict(flip_pairs(sizes[axis], shift, bit))[where[axis]]
                pairs.append(((z * nx + x) * nc + c, (where["z"] * nx + where["x"]) * nc + c))
    return lax.ppermute(value, SEG, pairs)


def swap_core(value):
    return lax.ppermute(value, "c", [(0, 1), (1, 0)])


def step_code(core, sizes):
    code = jnp.int32(0)
    for axis, shift, bit in STEPS[core][:-1]:
        ring = (lax.axis_index(axis) - shift + sizes[axis]) % sizes[axis]
        code = code * 2 + ((gray(ring) >> bit) & 1)
    return code * SUB


def sublane(shape=(CH, LANES)):
    return lax.broadcasted_iota(jnp.int32, shape, 0)


def down(v, k):
    return v if k == 0 else pltpu.roll(v, CH - k, 0)


def params():
    return pltpu.CompilerParams(vmem_limit_bytes=16 << 20)


def cost(blocks, flops):
    return pl.CostEstimate(flops=blocks * flops, bytes_accessed=0, transcendentals=0)


def block_of(code_ref, which, p):
    return code_ref[2 * which] + (p ^ code_ref[2 * which + 1])


def lanes_of(block):
    return pl.ds(pl.multiple_of(block * LANES, LANES), LANES)


def spectra_body(which, first, count, code_ref, valid_ref, mr_ref, mi_ref, hr_ref, hi_ref, out_ref):
    low = sublane() < 4
    keep = [valid_ref[s].astype(F32) for s in range(CH)]

    def step(p, carry):
        at = lanes_of(block_of(code_ref, which, first + p))
        acc = [jnp.zeros((CH, LANES), F32) for _ in range(12)]
        for s in range(CH):
            mr = mr_ref[s, :, at].astype(F32)
            mi = mi_ref[s, :, at].astype(F32)
            kr = mr * keep[s]
            ki = mi * keep[s]
            acc[0] = acc[0] + (kr * mr + ki * mi)
            for k in range(1, 4):
                rr = down(mr, k)
                ri = down(mi, k)
                acc[2 * k - 1] = acc[2 * k - 1] + (kr * rr + ki * ri)
                acc[2 * k] = acc[2 * k] + (ki * rr - kr * ri)
            rr = down(mr, 4)
            ri = down(mi, 4)
            acc[7] = acc[7] + (jnp.where(low, kr, ki) * rr + jnp.where(low, ki, -kr) * ri)
            hr = hr_ref[s, :, at].astype(F32)
            hi = hi_ref[s, :, at].astype(F32)
            for k in range(DET):
                br = jnp.broadcast_to(hr[k : k + 1], (CH, LANES))
                bi = jnp.broadcast_to(hi[k : k + 1], (CH, LANES))
                acc[8 + 2 * k] = acc[8 + 2 * k] + (kr * br + ki * bi)
                acc[9 + 2 * k] = acc[9 + 2 * k] + (ki * br - kr * bi)
        for r in range(12):
            out_ref[p, CH * r : CH * (r + 1), :] = acc[r]
        return carry

    lax.fori_loop(0, count, step, 0)


def spectra(codes, valid, mr, mi, hr, hi, which, first, count):
    return pl.pallas_call(
        lambda *refs: spectra_body(which, first, count, *refs),
        out_shape=jax.ShapeDtypeStruct((count, ROWS, LANES), F32),
        in_specs=[pl.BlockSpec(memory_space=SMEM)] * 2 + [pl.BlockSpec(memory_space=VMEM)] * 4,
        out_specs=pl.BlockSpec(memory_space=VMEM),
        compiler_params=params(),
        cost_estimate=cost(count, 500000),
        name="spectra",
    )(codes, valid, mr, mi, hr, hi)


def solve_block(rows):
    sub = sublane()
    low = sub < 4
    dr = [None] * CH
    di = [None] * CH
    dr[0] = rows[0] + 1.0
    di[0] = jnp.zeros_like(rows[0])
    for k in range(1, 4):
        dr[k], di[k] = rows[2 * k - 1], rows[2 * k]
        dr[CH - k] = pltpu.roll(rows[2 * k - 1], k, 0)
        di[CH - k] = -pltpu.roll(rows[2 * k], k, 0)
    half = rows[7]
    turned = pltpu.roll(half, 4, 0)
    dr[4] = jnp.where(low, half, turned)
    di[4] = jnp.where(low, -turned, half)
    cols_r, cols_i = [], []
    for j in range(CH):
        cr, ci = dr[j], di[j]
        for c in range(1, CH):
            cr = jnp.where(sub == c, dr[(j - c) % CH], cr)
            ci = jnp.where(sub == c, di[(j - c) % CH], ci)
        cols_r.append(cr)
        cols_i.append(ci)
    cols_r += [rows[8], rows[10]]
    cols_i += [rows[9], rows[11]]

    def row(v, j):
        return jnp.broadcast_to(v[j : j + 1], (CH, LANES))

    diag = jnp.ones((CH, LANES), F32)
    for j in range(CH):
        pivot = row(cols_r[j], j)
        diag = jnp.where(sub == j, pivot, diag)
        inv = 1.0 / pivot
        fr = jnp.where(sub == j, 0.0, cols_r[j] * inv)
        fi = jnp.where(sub == j, 0.0, cols_i[j] * inv)
        for k in range(j + 1, CH + DET):
            ar, ai = row(cols_r[k], j), row(cols_i[k], j)
            cols_r[k] = cols_r[k] - (fr * ar - fi * ai)
            cols_i[k] = cols_i[k] - (fr * ai + fi * ar)
    inv = 1.0 / diag
    return [cols_r[8] * inv, cols_i[8] * inv, cols_r[9] * inv, cols_i[9] * inv]


def solve_body(a_ref, b_ref, out_ref):
    for u in range(SUB):
        rows = [
            a_ref[u, CH * r : CH * (r + 1), :] + b_ref[u, CH * r : CH * (r + 1), :]
            for r in range(12)
        ]
        for q, tile in enumerate(solve_block(rows)):
            out_ref[u, CH * q : CH * (q + 1), :] = tile


def solve(a, b):
    return pl.pallas_call(
        solve_body,
        out_shape=jax.ShapeDtypeStruct((SUB, WROWS, LANES), F32),
        in_specs=[pl.BlockSpec(memory_space=VMEM)] * 2,
        out_specs=pl.BlockSpec(memory_space=VMEM),
        compiler_params=params(),
        cost_estimate=cost(SUB, 5000000),
        name="solve",
    )(a, b)


def channel_sums(tiles):
    sub = sublane()
    half = sub < 4
    level = []
    for s in range(4):
        a, b = tiles[s], tiles[s + 4]
        level.append(jnp.where(half, a, b) + pltpu.roll(jnp.where(half, b, a), 4, 0))
    for bit in (2, 1):
        mask = (sub & bit) == 0
        nxt = []
        for s in range(bit):
            a, b = level[s], level[s + bit]
            nxt.append(jnp.where(mask, a + pltpu.roll(a, CH - bit, 0), b + pltpu.roll(b, bit, 0)))
        level = nxt
    return level[0]


def clean_block(block, w, mr_ref, mi_ref, h_ref, inter_ref):
    at = lanes_of(block)
    parts = [[] for _ in range(4)]
    for s in range(CH):
        mr = mr_ref[s, :, at].astype(F32)
        mi = mi_ref[s, :, at].astype(F32)
        for k in range(DET):
            wr, wi = w[2 * k], w[2 * k + 1]
            parts[2 * k].append(wr * mr + wi * mi)
            parts[2 * k + 1].append(wr * mi - wi * mr)
    g = [h_ref[q, :, at] - channel_sums(parts[q]) for q in range(4)]
    real = g[0] * g[2] + g[1] * g[3]
    imag = g[1] * g[2] - g[0] * g[3]
    weight = jnp.broadcast_to(inter_ref[pl.ds(block, 1), :], (CH, LANES))
    return real, imag, real * weight


def filter_tiles(w_ref, p):
    return [w_ref[p, CH * q : CH * (q + 1), :] for q in range(4)]


def clean_body(which, first, count, code_ref, w_ref, mr_ref, mi_ref, h_ref, inter_ref, out_ref, num_ref):
    def step(p, num):
        block = block_of(code_ref, which, first + p)
        real, imag, part = clean_block(block, filter_tiles(w_ref, p), mr_ref, mi_ref, h_ref, inter_ref)
        out_ref[p, 0:CH, :] = real
        out_ref[p, CH : 2 * CH, :] = imag
        return num + part

    num_ref[...] = lax.fori_loop(0, count, step, jnp.zeros((CH, LANES), F32))


def clean(codes, filters, rest, which, first):
    count = filters.shape[0]
    return pl.pallas_call(
        lambda *refs: clean_body(which, first, count, *refs),
        out_shape=[
            jax.ShapeDtypeStruct((count, 2 * CH, LANES), F32),
            jax.ShapeDtypeStruct((CH, LANES), F32),
        ],
        in_specs=[pl.BlockSpec(memory_space=SMEM)] + [pl.BlockSpec(memory_space=VMEM)] * 5,
        out_specs=[pl.BlockSpec(memory_space=VMEM)] * 2,
        compiler_params=params(),
        cost_estimate=cost(count, 300000),
        name="clean",
    )(codes, filters, *rest)


def finish_body(which, first, count, places, code_ref, w_ref, mr_ref, mi_ref, h_ref, inter_ref, *refs):
    real_ref, imag_ref, num_ref = refs[-3:]
    done = refs[: len(places)]
    sums = refs[len(places) : 2 * len(places)]

    def step(p, num):
        block = block_of(code_ref, which, first + p)
        real, imag, part = clean_block(block, filter_tiles(w_ref, p), mr_ref, mi_ref, h_ref, inter_ref)
        at = lanes_of(block)
        real_ref[:, at] = real
        imag_ref[:, at] = imag
        return num + part

    num = lax.fori_loop(0, count, step, jnp.zeros((CH, LANES), F32))
    for (from_which, from_first), done_ref, sum_ref in zip(places, done, sums):
        num = num + sum_ref[...]

        def move(p, carry, from_which=from_which, from_first=from_first, done_ref=done_ref):
            at = lanes_of(block_of(code_ref, from_which, from_first + p))
            real_ref[:, at] = done_ref[p, 0:CH, :]
            imag_ref[:, at] = done_ref[p, CH : 2 * CH, :]
            return carry

        lax.fori_loop(0, done_ref.shape[0], move, 0, unroll=4)
    weight = inter_ref[...]
    square = jnp.sum(weight * weight)
    lane = lax.broadcasted_iota(jnp.int32, (CH, LANES), 1)
    total = jnp.broadcast_to(jnp.sum(num, axis=1, keepdims=True), (CH, LANES))
    num_ref[...] = jnp.where(lane == 0, total, square)


def finish(codes, filters, rest, which, first, places, pieces, sums):
    count = filters.shape[0]
    mr = rest[0]
    args = (codes, filters, *rest, *pieces, *sums)
    return pl.pallas_call(
        lambda *refs: finish_body(which, first, count, places, *refs),
        out_shape=[jax.ShapeDtypeStruct((mr.shape[0], mr.shape[2]), F32)] * 2
        + [jax.ShapeDtypeStruct((CH, LANES), F32)],
        in_specs=[pl.BlockSpec(memory_space=SMEM)]
        + [pl.BlockSpec(memory_space=VMEM)] * (len(args) - 1),
        out_specs=[pl.BlockSpec(memory_space=VMEM)] * 3,
        compiler_params=params(),
        cost_estimate=cost(count, 400000),
        name="finish",
    )(*args)


def summed_over_bin(value, sizes):
    for bit in range(sizes["y"].bit_length() - 1):
        value = value + lax.ppermute(value, "y", flip_pairs(sizes["y"], 0, bit))
    return value


def on_device(sizes, magnet_real, magnet_imag, detector_real, detector_imag, valid, intersection):
    bins = magnet_real.shape[2]
    half = bins // (LANES * sizes["c"])
    top = half // 2
    core = lax.axis_index("c")
    code_a, code_b = step_code(0, sizes), step_code(1, sizes)
    own = jnp.where(core == 0, code_a, code_b)
    other = jnp.where(core == 0, code_b, code_a)
    codes = jnp.stack([core * half, own, (1 - core) * half, other])
    data = (magnet_real, magnet_imag, detector_real, detector_imag)

    def reduced_over_core(first):
        away = spectra(codes, valid, *data, 1, first, top)
        away = swap_core(away)
        return [spectra(codes, valid, *data, 0, first, top), away]

    def summed(pieces, lo, hi):
        total = pieces[0][lo:hi]
        for piece in pieces[1:]:
            total = total + piece[lo:hi]
        return total

    pieces = reduced_over_core(top)
    got = swap_step(summed(pieces, 0, top), 0, sizes)
    pieces = reduced_over_core(0) + [got]
    h = jnp.stack([detector_real, detector_imag]).astype(F32)
    h = h.transpose(2, 0, 1, 3).reshape(2 * DET, CH, bins)
    size = top
    for at in range(1, len(STEPS[0]) - 1):
        size //= 2
        got = swap_step(summed(pieces, size, 2 * size), at, sizes)
        pieces = [p[:size] for p in pieces] + [got]
    last = summed(pieces, 0, size)
    got = swap_step(last, len(STEPS[0]) - 1, sizes)
    filters = solve(last, got)

    rest = (magnet_real, magnet_imag, h, intersection.reshape(bins // LANES, LANES))
    for at in range(len(STEPS[0]) - 2, 0, -1):
        filters = jnp.concatenate([filters, swap_step(filters, at, sizes)], axis=0)
    upper = swap_step(filters, 0, sizes)
    other = swap_core(filters)
    last = swap_core(upper)
    pieces, sums = [], []
    places = ((0, 0), (1, 0), (0, top))
    for f, place in zip((filters, other, upper), places):
        piece, num = clean(codes, f, rest, *place)
        pieces.append(piece)
        sums.append(num)
    real, imag, num = finish(codes, last, rest, 1, top, places, pieces, sums)
    totals = summed_over_bin(num, sizes)
    estimate = totals[:, 0] / jnp.sqrt(totals[:, 1])
    return (real, imag, estimate)


def solution(mesh):
    sizes = {"z": 8, "x": 4, "c": 2, "y": mesh.shape["bin"]}
    torus = Mesh(mesh.devices.reshape(*sizes.values()), tuple(sizes))
    in_specs = (
        P(SEG, None, "y"),
        P(SEG, None, "y"),
        P(SEG, None, "y"),
        P(SEG, None, "y"),
        P(SEG),
        P("y"),
    )
    out_specs = (P(SEG, "y"), P(SEG, "y"), P(SEG))

    def body(*args):
        return on_device(sizes, *args)

    return jax.shard_map(
        body, mesh=torus, in_specs=in_specs, out_specs=out_specs, check_vma=False
    )
```

```python
import jax
import jax.numpy as jnp
from jax import lax
from jax.experimental import pallas as pl
from jax.experimental.pallas import tpu as pltpu
from jax.sharding import Mesh
from jax.sharding import PartitionSpec as P


SEG = ("z", "x", "c")
LANES = 128
CH = 8
DET = 2
ROWS = 96
WROWS = 32
VMEM = pltpu.VMEM
F32 = jnp.float32


def gray(i):
    return i ^ (i >> 1)


def flip_pairs(size, shift, bit):
    where = {gray((i - shift) % size): i for i in range(size)}
    return [(i, where[gray((i - shift) % size) ^ (1 << bit)]) for i in range(size)]


STEPS = (
    (("x", 0, 0), ("x", 0, 1), ("z", 0, 0), ("z", 0, 1), ("z", 0, 2)),
    (("x", 0, 1), ("x", 0, 0), ("z", 1, 0), ("z", 1, 2), ("z", 1, 1)),
)
SUB = 2


def swap_steps(value, steps, sizes):
    nz, nx, nc = sizes["z"], sizes["x"], sizes["c"]
    pairs = []
    for z in range(nz):
        for x in range(nx):
            for c in range(nc):
                where = {"z": z, "x": x}
                for at in steps:
                    axis, shift, bit = STEPS[c][at]
                    where[axis] = dict(flip_pairs(sizes[axis], shift, bit))[where[axis]]
                pairs.append(((z * nx + x) * nc + c, (where["z"] * nx + where["x"]) * nc + c))
    return lax.ppermute(value, SEG, pairs)


def swap_core(value):
    return lax.ppermute(value, "c", [(0, 1), (1, 0)])


def step_code(core, sizes):
    code = jnp.int32(0)
    for axis, shift, bit in STEPS[core][:-1]:
        ring = (lax.axis_index(axis) + (sizes[axis] - shift)) & (sizes[axis] - 1)
        code = code * 2 + ((gray(ring) >> bit) & 1)
    return code * SUB


def half_codes(sizes, half):
    core = lax.axis_index("c")
    code_a, code_b = step_code(0, sizes), step_code(1, sizes)
    own = jnp.where(core == 0, code_a, code_b)
    other = jnp.where(core == 0, code_b, code_a)
    return ((core * half, own), ((1 - core) * half, other))


def sublane(shape=(CH, LANES)):
    return lax.broadcasted_iota(jnp.int32, shape, 0)


def down(v, k):
    return v if k == 0 else pltpu.roll(v, CH - k, 0)


def params():
    return pltpu.CompilerParams(vmem_limit_bytes=16 << 20)


def cost(blocks, flops):
    return pl.CostEstimate(flops=blocks * flops, bytes_accessed=0, transcendentals=0)


def block_of(codes, which, p):
    base, code = codes[which]
    return base + (p ^ code)


def lanes_of(block):
    return pl.ds(pl.multiple_of(block * LANES, LANES), LANES)


def spectra_block(at, keep, mr_ref, mi_ref, hr_ref, hi_ref, store):
    low = sublane() < 4
    acc = [jnp.zeros((CH, LANES), F32) for _ in range(12)]
    for s in range(CH):
        mr = mr_ref[s, :, at].astype(F32)
        mi = mi_ref[s, :, at].astype(F32)
        kr = mr * keep[s]
        ki = mi * keep[s]
        acc[0] = acc[0] + (kr * mr + ki * mi)
        for k in range(1, 4):
            rr = down(mr, k)
            ri = down(mi, k)
            acc[2 * k - 1] = acc[2 * k - 1] + (kr * rr + ki * ri)
            acc[2 * k] = acc[2 * k] + (ki * rr - kr * ri)
        rr = down(mr, 4)
        ri = down(mi, 4)
        acc[7] = acc[7] + (jnp.where(low, kr, ki) * rr + jnp.where(low, ki, -kr) * ri)
        hr = hr_ref[s, :, at].astype(F32)
        hi = hi_ref[s, :, at].astype(F32)
        for k in range(DET):
            br = jnp.broadcast_to(hr[k : k + 1], (CH, LANES))
            bi = jnp.broadcast_to(hi[k : k + 1], (CH, LANES))
            acc[8 + 2 * k] = acc[8 + 2 * k] + (kr * br + ki * bi)
            acc[9 + 2 * k] = acc[9 + 2 * k] + (ki * br - kr * bi)
    for r in range(12):
        store(r, acc[r])


def spectra_loop(codes, which, first, count, keep, data, out_ref):
    def step(p, carry):
        def store(r, tile):
            out_ref[p, CH * r : CH * (r + 1), :] = tile

        spectra_block(lanes_of(block_of(codes, which, first + p)), keep, *data, store)
        return carry

    lax.fori_loop(0, count, step, 0)


def front_body(sizes, half, first, count, valid_hbm, *refs):
    hbm, (out_ref, keep_ref, *local) = refs[:4], refs[4:10]
    keep_smem, keep_sem, sems = refs[10:]
    codes = half_codes(sizes, half)
    width = count * LANES
    npiece = hbm[0].shape[2] // width
    lead = block_of(codes, 1, first) // count
    keep_copy = pltpu.make_async_copy(valid_hbm, keep_smem, keep_sem)
    keep_copy.start()
    copies = []
    for n in range(npiece):
        at = pl.ds(pl.multiple_of((n ^ lead) * width, width), width)
        copies.append(
            [
                pltpu.make_async_copy(src.at[:, :, at], dst.at[:, :, at], sems.at[n, i])
                for i, (src, dst) in enumerate(zip(hbm, local))
            ]
        )
        for copy in copies[-1]:
            copy.start()
    keep_copy.wait()
    for copy in copies[0]:
        copy.wait()
    for s in range(CH):
        keep_ref[s] = jnp.full((CH, LANES), keep_smem[s].astype(F32))
    spectra_loop(codes, 1, first, count, keep_ref, local, out_ref)
    for piece in copies[1:]:
        for copy in piece:
            copy.wait()


def front(sizes, half, valid, data, first, count):
    npiece = data[0].shape[2] // (count * LANES)
    return pl.pallas_call(
        lambda *refs: front_body(sizes, half, first, count, *refs),
        out_shape=[
            jax.ShapeDtypeStruct((count, ROWS, LANES), F32),
            jax.ShapeDtypeStruct((CH, CH, LANES), F32),
        ]
        + [jax.ShapeDtypeStruct(d.shape, d.dtype) for d in data],
        in_specs=[pl.BlockSpec(memory_space=pltpu.MemorySpace.HBM)] * 5,
        out_specs=[pl.BlockSpec(memory_space=VMEM)] * 6,
        scratch_shapes=[
            pltpu.SMEM(valid.shape, valid.dtype),
            pltpu.SemaphoreType.DMA,
            pltpu.SemaphoreType.DMA((npiece, 4)),
        ],
        compiler_params=params(),
        cost_estimate=cost(count, 500000),
        name="front",
    )(*(pltpu.with_memory_space_constraint(a, pltpu.MemorySpace.HBM) for a in (valid, *data)))


def spectra_body(sizes, half, which, first, count, keep_ref, *refs):
    spectra_loop(half_codes(sizes, half), which, first, count, keep_ref, refs[:4], refs[4])


def spectra(sizes, half, keep, data, which, first, count):
    return pl.pallas_call(
        lambda *refs: spectra_body(sizes, half, which, first, count, *refs),
        out_shape=jax.ShapeDtypeStruct((count, ROWS, LANES), F32),
        in_specs=[pl.BlockSpec(memory_space=VMEM)] * 5,
        out_specs=pl.BlockSpec(memory_space=VMEM),
        compiler_params=params(),
        cost_estimate=cost(count, 500000),
        name="spectra",
    )(keep, *data)


def solve_block(rows):
    sub = sublane()
    low = sub < 4
    dr = [None] * CH
    di = [None] * CH
    dr[0] = rows[0] + 1.0
    di[0] = jnp.zeros_like(rows[0])
    for k in range(1, 4):
        dr[k], di[k] = rows[2 * k - 1], rows[2 * k]
        dr[CH - k] = pltpu.roll(rows[2 * k - 1], k, 0)
        di[CH - k] = -pltpu.roll(rows[2 * k], k, 0)
    half = rows[7]
    turned = pltpu.roll(half, 4, 0)
    dr[4] = jnp.where(low, half, turned)
    di[4] = jnp.where(low, -turned, half)
    cols_r, cols_i = [], []
    for j in range(CH):
        cr, ci = dr[j], di[j]
        for c in range(1, CH):
            cr = jnp.where(sub == c, dr[(j - c) % CH], cr)
            ci = jnp.where(sub == c, di[(j - c) % CH], ci)
        cols_r.append(cr)
        cols_i.append(ci)
    cols_r += [rows[8], rows[10]]
    cols_i += [rows[9], rows[11]]

    def row(v, j):
        return jnp.broadcast_to(v[j : j + 1], (CH, LANES))

    diag = jnp.ones((CH, LANES), F32)
    for j in range(CH):
        pivot = row(cols_r[j], j)
        diag = jnp.where(sub == j, pivot, diag)
        inv = 1.0 / pivot
        fr = jnp.where(sub == j, 0.0, cols_r[j] * inv)
        fi = jnp.where(sub == j, 0.0, cols_i[j] * inv)
        for k in range(j + 1, CH + DET):
            ar, ai = row(cols_r[k], j), row(cols_i[k], j)
            cols_r[k] = cols_r[k] - (fr * ar - fi * ai)
            cols_i[k] = cols_i[k] - (fr * ai + fi * ar)
    inv = 1.0 / diag
    return [cols_r[8] * inv, cols_i[8] * inv, cols_r[9] * inv, cols_i[9] * inv]


def solve_body(a_ref, b_ref, out_ref):
    for u in range(SUB):
        rows = [
            a_ref[u, CH * r : CH * (r + 1), :] + b_ref[u, CH * r : CH * (r + 1), :]
            for r in range(12)
        ]
        for q, tile in enumerate(solve_block(rows)):
            out_ref[u, CH * q : CH * (q + 1), :] = tile


def solve(a, b):
    return pl.pallas_call(
        solve_body,
        out_shape=jax.ShapeDtypeStruct((SUB, WROWS, LANES), F32),
        in_specs=[pl.BlockSpec(memory_space=VMEM)] * 2,
        out_specs=pl.BlockSpec(memory_space=VMEM),
        compiler_params=params(),
        cost_estimate=cost(SUB, 5000000),
        name="solve",
    )(a, b)


def channel_sums(tiles):
    sub = sublane()
    half = sub < 4
    level = []
    for s in range(4):
        a, b = tiles[s], tiles[s + 4]
        level.append(jnp.where(half, a, b) + pltpu.roll(jnp.where(half, b, a), 4, 0))
    for bit in (2, 1):
        mask = (sub & bit) == 0
        nxt = []
        for s in range(bit):
            a, b = level[s], level[s + bit]
            nxt.append(jnp.where(mask, a + pltpu.roll(a, CH - bit, 0), b + pltpu.roll(b, bit, 0)))
        level = nxt
    return level[0]


def clean_block(block, w, mr_ref, mi_ref, h_ref, inter_ref):
    at = lanes_of(block)
    parts = [[] for _ in range(4)]
    for s in range(CH):
        mr = mr_ref[s, :, at].astype(F32)
        mi = mi_ref[s, :, at].astype(F32)
        for k in range(DET):
            wr, wi = w[2 * k], w[2 * k + 1]
            parts[2 * k].append(wr * mr + wi * mi)
            parts[2 * k + 1].append(wr * mi - wi * mr)
    g = [h_ref[q, :, at] - channel_sums(parts[q]) for q in range(4)]
    real = g[0] * g[2] + g[1] * g[3]
    imag = g[1] * g[2] - g[0] * g[3]
    weight = jnp.broadcast_to(inter_ref[pl.ds(block, 1), :], (CH, LANES))
    return real, imag, real * weight


def filter_tiles(w_ref, p):
    return [w_ref[p, CH * q : CH * (q + 1), :] for q in range(4)]


def clean_body(sizes, half, which, first, count, w_ref, *refs):
    data, (out_ref, num_ref) = refs[:4], refs[4:]
    codes = half_codes(sizes, half)

    def step(p, num):
        block = block_of(codes, which, first + p)
        real, imag, part = clean_block(block, filter_tiles(w_ref, p), *data)
        out_ref[p, 0:CH, :] = real
        out_ref[p, CH : 2 * CH, :] = imag
        return num + part

    num_ref[...] = lax.fori_loop(0, count, step, jnp.zeros((CH, LANES), F32))


def clean(sizes, half, filters, rest, which, first):
    count = filters.shape[0]
    return pl.pallas_call(
        lambda *refs: clean_body(sizes, half, which, first, count, *refs),
        out_shape=[
            jax.ShapeDtypeStruct((count, 2 * CH, LANES), F32),
            jax.ShapeDtypeStruct((CH, LANES), F32),
        ],
        in_specs=[pl.BlockSpec(memory_space=VMEM)] * 5,
        out_specs=[pl.BlockSpec(memory_space=VMEM)] * 2,
        compiler_params=params(),
        cost_estimate=cost(count, 300000),
        name="clean",
    )(filters, *rest)


def finish_body(sizes, half, which, first, count, places, w_ref, *refs):
    data, refs = refs[:4], refs[4:]
    real_ref, imag_ref, num_ref = refs[-3:]
    done = refs[: len(places)]
    sums = refs[len(places) : 2 * len(places)]
    codes = half_codes(sizes, half)

    def step(p, num):
        block = block_of(codes, which, first + p)
        real, imag, part = clean_block(block, filter_tiles(w_ref, p), *data)
        at = lanes_of(block)
        real_ref[:, at] = real
        imag_ref[:, at] = imag
        return num + part

    num = lax.fori_loop(0, count, step, jnp.zeros((CH, LANES), F32))
    for (from_which, from_first), done_ref, sum_ref in zip(places, done, sums):
        num = num + sum_ref[...]
        for p in range(done_ref.shape[0]):
            at = lanes_of(block_of(codes, from_which, from_first + p))
            real_ref[:, at] = done_ref[p, 0:CH, :]
            imag_ref[:, at] = done_ref[p, CH : 2 * CH, :]
    weight = data[3][...]
    square = jnp.sum(weight * weight)
    lane = lax.broadcasted_iota(jnp.int32, (CH, LANES), 1)
    total = jnp.broadcast_to(jnp.sum(num, axis=1, keepdims=True), (CH, LANES))
    num_ref[...] = jnp.where(lane == 0, total, square)


def finish(sizes, half, filters, rest, which, first, places, pieces, sums):
    count = filters.shape[0]
    mr = rest[0]
    args = (filters, *rest, *pieces, *sums)
    return pl.pallas_call(
        lambda *refs: finish_body(sizes, half, which, first, count, places, *refs),
        out_shape=[jax.ShapeDtypeStruct((mr.shape[0], mr.shape[2]), F32)] * 2
        + [jax.ShapeDtypeStruct((CH, LANES), F32)],
        in_specs=[pl.BlockSpec(memory_space=VMEM)] * len(args),
        out_specs=[pl.BlockSpec(memory_space=VMEM)] * 3,
        compiler_params=params(),
        cost_estimate=cost(count, 400000),
        name="finish",
    )(*args)


def summed_over_bin(value, sizes):
    for bit in range(sizes["y"].bit_length() - 1):
        value = value + lax.ppermute(value, "y", flip_pairs(sizes["y"], 0, bit))
    return value


def on_device(sizes, magnet_real, magnet_imag, detector_real, detector_imag, valid, intersection):
    bins = magnet_real.shape[2]
    half = bins // (LANES * sizes["c"])
    q = half // 4
    e = half // 8
    data = (magnet_real, magnet_imag, detector_real, detector_imag)

    away, keep, *data = front(sizes, half, valid, data, 3 * q, q)
    received = []

    def local(first, count, away=None):
        if away is None:
            away = spectra(sizes, half, keep, data, 1, first, count)
        away = swap_core(away)
        own = spectra(sizes, half, keep, data, 0, first, count)
        received.extend([(first, first + count, own), (first, first + count, away)])

    def summed(lo, hi):
        parts = [a[lo - f : hi - f] for f, t, a in received if f <= lo and hi <= t]
        total = parts[0]
        for part in parts[1:]:
            total = total + part
        return total

    def halve(at, lo, hi, to):
        got = swap_steps(summed(lo, hi), (at,), sizes)
        received.append((to, to + hi - lo, got))

    local(3 * q, q, away)
    halve(0, 3 * q, 4 * q, q)
    local(2 * q, q)
    halve(0, 2 * q, 3 * q, 0)
    local(0, 2 * q)
    h = jnp.stack([data[2], data[3]]).astype(F32)
    h = h.transpose(2, 0, 1, 3).reshape(2 * DET, CH, bins)
    halve(1, 3 * e, 4 * e, e)
    halve(1, 2 * e, 3 * e, 0)
    halve(2, e, 2 * e, 0)
    halve(3, e // 2, e, 0)
    last = summed(0, SUB)
    got = swap_steps(last, (4,), sizes)
    filters = solve(last, got)

    rest = (data[0], data[1], h, intersection.reshape(bins // LANES, LANES))
    near = [filters]
    for steps in ((3,), (2,), (2, 3)):
        near.append(swap_steps(filters, steps, sizes))
    near = jnp.concatenate(near, axis=0)
    quarters = [near]
    quarters.append(swap_steps(near, (1,), sizes))
    quarters.append(swap_steps(near, (0,), sizes))
    quarters.append(swap_steps(quarters[1], (0,), sizes))
    pieces, sums, places = [], [], []
    for n, mine in enumerate(quarters):
        other = swap_core(mine)
        for which, filt in enumerate((mine, other)):
            if (n, which) == (3, 1):
                real, imag, num = finish(
                    sizes, half, filt, rest, which, n * q, places, pieces, sums
                )
            else:
                piece, num = clean(sizes, half, filt, rest, which, n * q)
                pieces.append(piece)
                sums.append(num)
                places.append((which, n * q))
    totals = summed_over_bin(num, sizes)
    estimate = totals[:, 0] / jnp.sqrt(totals[:, 1])
    return (real, imag, estimate)


def solution(mesh):
    sizes = {"z": 8, "x": 4, "c": 2, "y": mesh.shape["bin"]}
    torus = Mesh(mesh.devices.reshape(*sizes.values()), tuple(sizes))
    in_specs = (
        P(SEG, None, "y"),
        P(SEG, None, "y"),
        P(SEG, None, "y"),
        P(SEG, None, "y"),
        P(SEG),
        P("y"),
    )
    out_specs = (P(SEG, "y"), P(SEG, "y"), P(SEG))

    def body(*args):
        return on_device(sizes, *args)

    return jax.shard_map(
        body, mesh=torus, in_specs=in_specs, out_specs=out_specs, check_vma=False
    )
```

```python
import jax
import jax.numpy as jnp
from jax import lax
from jax.experimental import pallas as pl
from jax.experimental.pallas import tpu as pltpu
from jax.sharding import Mesh
from jax.sharding import PartitionSpec as P


SEG = ("z", "x", "c")
LANES = 128
CH = 8
DET = 2
ROWS = 96
WROWS = 32
VMEM = pltpu.VMEM
F32 = jnp.float32


def gray(i):
    return i ^ (i >> 1)


def label(axis, i):
    return (gray(i >> 1) << 1) | (i & 1) if axis == "z" else gray(i)


def flip_pairs(axis, size, shift, bits):
    where = {label(axis, (i - shift) % size): i for i in range(size)}
    return [(i, where[label(axis, (i - shift) % size) ^ bits]) for i in range(size)]


STEPS = (
    (("x", 0, 0), ("x", 0, 1), ("z", 0, 0), ("z", 0, 1), ("z", 0, 2)),
    (("x", 0, 1), ("x", 0, 0), ("z", 1, 0), ("z", 1, 2), ("z", 1, 1)),
)
SUB = 2


def swap_steps(value, steps, sizes):
    nz, nx, nc = sizes["z"], sizes["x"], sizes["c"]
    pairs = []
    for z in range(nz):
        for x in range(nx):
            for c in range(nc):
                where = {"z": z, "x": x}
                for at in steps:
                    axis, shift, bit = STEPS[c][at]
                    where[axis] = dict(flip_pairs(axis, sizes[axis], shift, 1 << bit))[where[axis]]
                pairs.append(((z * nx + x) * nc + c, (where["z"] * nx + where["x"]) * nc + c))
    return lax.ppermute(value, SEG, pairs)


def swap_core(value):
    return lax.ppermute(value, "c", [(0, 1), (1, 0)])


def step_code(core, sizes):
    code = jnp.int32(0)
    for axis, shift, bit in STEPS[core][:-1]:
        ring = (lax.axis_index(axis) + (sizes[axis] - shift)) & (sizes[axis] - 1)
        code = code * 2 + ((label(axis, ring) >> bit) & 1)
    return code * SUB


def half_codes(sizes, half):
    core = lax.axis_index("c")
    code_a, code_b = step_code(0, sizes), step_code(1, sizes)
    own = jnp.where(core == 0, code_a, code_b)
    other = jnp.where(core == 0, code_b, code_a)
    return ((core * half, own), ((1 - core) * half, other))


def sublane(shape=(CH, LANES)):
    return lax.broadcasted_iota(jnp.int32, shape, 0)


def down(v, k):
    return v if k == 0 else pltpu.roll(v, CH - k, 0)


def params():
    return pltpu.CompilerParams(vmem_limit_bytes=16 << 20)


def cost(blocks, flops):
    return pl.CostEstimate(flops=blocks * flops, bytes_accessed=0, transcendentals=0)


def block_of(codes, which, p):
    base, code = codes[which]
    return base + (p ^ code)


def lanes_of(block):
    return pl.ds(pl.multiple_of(block * LANES, LANES), LANES)


def spectra_block(at, keep, mr_ref, mi_ref, hr_ref, hi_ref, store):
    low = sublane() < 4
    acc = [jnp.zeros((CH, LANES), F32) for _ in range(12)]
    for s in range(CH):
        mr = mr_ref[s, :, at].astype(F32)
        mi = mi_ref[s, :, at].astype(F32)
        kr = mr * keep[s]
        ki = mi * keep[s]
        acc[0] = acc[0] + (kr * mr + ki * mi)
        for k in range(1, 4):
            rr = down(mr, k)
            ri = down(mi, k)
            acc[2 * k - 1] = acc[2 * k - 1] + (kr * rr + ki * ri)
            acc[2 * k] = acc[2 * k] + (ki * rr - kr * ri)
        rr = down(mr, 4)
        ri = down(mi, 4)
        acc[7] = acc[7] + (jnp.where(low, kr, ki) * rr + jnp.where(low, ki, -kr) * ri)
        hr = hr_ref[s, :, at].astype(F32)
        hi = hi_ref[s, :, at].astype(F32)
        for k in range(DET):
            br = jnp.broadcast_to(hr[k : k + 1], (CH, LANES))
            bi = jnp.broadcast_to(hi[k : k + 1], (CH, LANES))
            acc[8 + 2 * k] = acc[8 + 2 * k] + (kr * br + ki * bi)
            acc[9 + 2 * k] = acc[9 + 2 * k] + (ki * br - kr * bi)
    for r in range(12):
        store(r, acc[r])


def spectra_loop(codes, which, first, count, keep, data, out_ref):
    def step(p, carry):
        def store(r, tile):
            out_ref[p, CH * r : CH * (r + 1), :] = tile

        spectra_block(lanes_of(block_of(codes, which, first + p)), keep, *data, store)
        return carry

    lax.fori_loop(0, count, step, 0)


def front_body(sizes, half, first, count, valid_hbm, *refs):
    hbm, (out_ref, keep_ref, *local) = refs[:4], refs[4:10]
    keep_smem, keep_sem, sems = refs[10:]
    codes = half_codes(sizes, half)
    width = count * LANES
    npiece = hbm[0].shape[2] // width
    lead = block_of(codes, 1, first) // count
    keep_copy = pltpu.make_async_copy(valid_hbm, keep_smem, keep_sem)
    keep_copy.start()
    copies = []
    for n in range(npiece):
        at = pl.ds(pl.multiple_of((n ^ lead) * width, width), width)
        copies.append(
            [
                pltpu.make_async_copy(src.at[:, :, at], dst.at[:, :, at], sems.at[n, i])
                for i, (src, dst) in enumerate(zip(hbm, local))
            ]
        )
        for copy in copies[-1]:
            copy.start()
    keep_copy.wait()
    for copy in copies[0]:
        copy.wait()
    for s in range(CH):
        keep_ref[s] = jnp.full((CH, LANES), keep_smem[s].astype(F32))
    spectra_loop(codes, 1, first, count, keep_ref, local, out_ref)
    for piece in copies[1:]:
        for copy in piece:
            copy.wait()


def front(sizes, half, valid, data, first, count):
    npiece = data[0].shape[2] // (count * LANES)
    return pl.pallas_call(
        lambda *refs: front_body(sizes, half, first, count, *refs),
        out_shape=[
            jax.ShapeDtypeStruct((count, ROWS, LANES), F32),
            jax.ShapeDtypeStruct((CH, CH, LANES), F32),
        ]
        + [jax.ShapeDtypeStruct(d.shape, d.dtype) for d in data],
        in_specs=[pl.BlockSpec(memory_space=pltpu.MemorySpace.HBM)] * 5,
        out_specs=[pl.BlockSpec(memory_space=VMEM)] * 6,
        scratch_shapes=[
            pltpu.SMEM(valid.shape, valid.dtype),
            pltpu.SemaphoreType.DMA,
            pltpu.SemaphoreType.DMA((npiece, 4)),
        ],
        compiler_params=params(),
        cost_estimate=cost(count, 500000),
        name="front",
    )(*(pltpu.with_memory_space_constraint(a, pltpu.MemorySpace.HBM) for a in (valid, *data)))


def spectra_body(sizes, half, which, first, count, keep_ref, *refs):
    spectra_loop(half_codes(sizes, half), which, first, count, keep_ref, refs[:4], refs[4])


def spectra(sizes, half, keep, data, which, first, count):
    return pl.pallas_call(
        lambda *refs: spectra_body(sizes, half, which, first, count, *refs),
        out_shape=jax.ShapeDtypeStruct((count, ROWS, LANES), F32),
        in_specs=[pl.BlockSpec(memory_space=VMEM)] * 5,
        out_specs=pl.BlockSpec(memory_space=VMEM),
        compiler_params=params(),
        cost_estimate=cost(count, 500000),
        name="spectra",
    )(keep, *data)


def solve_block(rows):
    sub = sublane()
    low = sub < 4
    dr = [None] * CH
    di = [None] * CH
    dr[0] = rows[0] + 1.0
    di[0] = jnp.zeros_like(rows[0])
    for k in range(1, 4):
        dr[k], di[k] = rows[2 * k - 1], rows[2 * k]
        dr[CH - k] = pltpu.roll(rows[2 * k - 1], k, 0)
        di[CH - k] = -pltpu.roll(rows[2 * k], k, 0)
    half = rows[7]
    turned = pltpu.roll(half, 4, 0)
    dr[4] = jnp.where(low, half, turned)
    di[4] = jnp.where(low, -turned, half)
    cols_r, cols_i = [], []
    for j in range(CH):
        cr, ci = dr[j], di[j]
        for c in range(1, CH):
            cr = jnp.where(sub == c, dr[(j - c) % CH], cr)
            ci = jnp.where(sub == c, di[(j - c) % CH], ci)
        cols_r.append(cr)
        cols_i.append(ci)
    cols_r += [rows[8], rows[10]]
    cols_i += [rows[9], rows[11]]

    def row(v, j):
        return jnp.broadcast_to(v[j : j + 1], (CH, LANES))

    diag = jnp.ones((CH, LANES), F32)
    for j in range(CH):
        pivot = row(cols_r[j], j)
        diag = jnp.where(sub == j, pivot, diag)
        inv = 1.0 / pivot
        fr = jnp.where(sub == j, 0.0, cols_r[j] * inv)
        fi = jnp.where(sub == j, 0.0, cols_i[j] * inv)
        for k in range(j + 1, CH + DET):
            ar, ai = row(cols_r[k], j), row(cols_i[k], j)
            cols_r[k] = cols_r[k] - (fr * ar - fi * ai)
            cols_i[k] = cols_i[k] - (fr * ai + fi * ar)
    inv = 1.0 / diag
    return [cols_r[8] * inv, cols_i[8] * inv, cols_r[9] * inv, cols_i[9] * inv]


def solve_body(a_ref, b_ref, out_ref):
    for u in range(SUB):
        rows = [
            a_ref[u, CH * r : CH * (r + 1), :] + b_ref[u, CH * r : CH * (r + 1), :]
            for r in range(12)
        ]
        for q, tile in enumerate(solve_block(rows)):
            out_ref[u, CH * q : CH * (q + 1), :] = tile


def solve(a, b):
    return pl.pallas_call(
        solve_body,
        out_shape=jax.ShapeDtypeStruct((SUB, WROWS, LANES), F32),
        in_specs=[pl.BlockSpec(memory_space=VMEM)] * 2,
        out_specs=pl.BlockSpec(memory_space=VMEM),
        compiler_params=params(),
        cost_estimate=cost(SUB, 5000000),
        name="solve",
    )(a, b)


def channel_sums(tiles):
    sub = sublane()
    half = sub < 4
    level = []
    for s in range(4):
        a, b = tiles[s], tiles[s + 4]
        level.append(jnp.where(half, a, b) + pltpu.roll(jnp.where(half, b, a), 4, 0))
    for bit in (2, 1):
        mask = (sub & bit) == 0
        nxt = []
        for s in range(bit):
            a, b = level[s], level[s + bit]
            nxt.append(jnp.where(mask, a + pltpu.roll(a, CH - bit, 0), b + pltpu.roll(b, bit, 0)))
        level = nxt
    return level[0]


def clean_block(block, w, mr_ref, mi_ref, h_ref, inter_ref):
    at = lanes_of(block)
    parts = [[] for _ in range(4)]
    for s in range(CH):
        mr = mr_ref[s, :, at].astype(F32)
        mi = mi_ref[s, :, at].astype(F32)
        for k in range(DET):
            wr, wi = w[2 * k], w[2 * k + 1]
            parts[2 * k].append(wr * mr + wi * mi)
            parts[2 * k + 1].append(wr * mi - wi * mr)
    g = [h_ref[q, :, at] - channel_sums(parts[q]) for q in range(4)]
    real = g[0] * g[2] + g[1] * g[3]
    imag = g[1] * g[2] - g[0] * g[3]
    weight = jnp.broadcast_to(inter_ref[pl.ds(block, 1), :], (CH, LANES))
    return real, imag, real * weight


def filter_tiles(w_ref, p):
    return [w_ref[p, CH * q : CH * (q + 1), :] for q in range(4)]


def clean_body(sizes, half, which, first, count, w_ref, *refs):
    data, (out_ref, num_ref) = refs[:4], refs[4:]
    codes = half_codes(sizes, half)

    def step(p, num):
        block = block_of(codes, which, first + p)
        real, imag, part = clean_block(block, filter_tiles(w_ref, p), *data)
        out_ref[p, 0:CH, :] = real
        out_ref[p, CH : 2 * CH, :] = imag
        return num + part

    num_ref[...] = lax.fori_loop(0, count, step, jnp.zeros((CH, LANES), F32))


def clean(sizes, half, filters, rest, which, first):
    count = filters.shape[0]
    return pl.pallas_call(
        lambda *refs: clean_body(sizes, half, which, first, count, *refs),
        out_shape=[
            jax.ShapeDtypeStruct((count, 2 * CH, LANES), F32),
            jax.ShapeDtypeStruct((CH, LANES), F32),
        ],
        in_specs=[pl.BlockSpec(memory_space=VMEM)] * 5,
        out_specs=[pl.BlockSpec(memory_space=VMEM)] * 2,
        compiler_params=params(),
        cost_estimate=cost(count, 300000),
        name="clean",
    )(filters, *rest)


def finish_body(sizes, half, which, first, count, places, w_ref, *refs):
    data, refs = refs[:4], refs[4:]
    real_ref, imag_ref, num_ref = refs[-3:]
    done = refs[: len(places)]
    sums = refs[len(places) : 2 * len(places)]
    codes = half_codes(sizes, half)

    def step(p, num):
        block = block_of(codes, which, first + p)
        real, imag, part = clean_block(block, filter_tiles(w_ref, p), *data)
        at = lanes_of(block)
        real_ref[:, at] = real
        imag_ref[:, at] = imag
        return num + part

    num = lax.fori_loop(0, count, step, jnp.zeros((CH, LANES), F32))
    for (from_which, from_first), done_ref, sum_ref in zip(places, done, sums):
        num = num + sum_ref[...]
        for p in range(done_ref.shape[0]):
            at = lanes_of(block_of(codes, from_which, from_first + p))
            real_ref[:, at] = done_ref[p, 0:CH, :]
            imag_ref[:, at] = done_ref[p, CH : 2 * CH, :]
    weight = data[3][...]
    square = jnp.sum(weight * weight)
    lane = lax.broadcasted_iota(jnp.int32, (CH, LANES), 1)
    total = jnp.broadcast_to(jnp.sum(num, axis=1, keepdims=True), (CH, LANES))
    num_ref[...] = jnp.where(lane == 0, total, square)


def finish(sizes, half, filters, rest, which, first, places, pieces, sums):
    count = filters.shape[0]
    mr = rest[0]
    args = (filters, *rest, *pieces, *sums)
    return pl.pallas_call(
        lambda *refs: finish_body(sizes, half, which, first, count, places, *refs),
        out_shape=[jax.ShapeDtypeStruct((mr.shape[0], mr.shape[2]), F32)] * 2
        + [jax.ShapeDtypeStruct((CH, LANES), F32)],
        in_specs=[pl.BlockSpec(memory_space=VMEM)] * len(args),
        out_specs=[pl.BlockSpec(memory_space=VMEM)] * 3,
        compiler_params=params(),
        cost_estimate=cost(count, 400000),
        name="finish",
    )(*args)


def summed_over_bin(value, sizes):
    got = [value]
    for bits in range(1, sizes["y"]):
        got.append(lax.ppermute(value, "y", flip_pairs("y", sizes["y"], 0, bits)))
    while len(got) > 1:
        got = [a + b for a, b in zip(got[::2], got[1::2])]
    return got[0]


def on_device(sizes, magnet_real, magnet_imag, detector_real, detector_imag, valid, intersection):
    bins = magnet_real.shape[2]
    half = bins // (LANES * sizes["c"])
    q = half // 4
    e = half // 8
    data = (magnet_real, magnet_imag, detector_real, detector_imag)

    away, keep, *data = front(sizes, half, valid, data, 3 * q, q)
    received = []

    def local(first, count, away=None):
        if away is None:
            away = spectra(sizes, half, keep, data, 1, first, count)
        away = swap_core(away)
        own = spectra(sizes, half, keep, data, 0, first, count)
        received.extend([(first, first + count, own), (first, first + count, away)])

    def summed(lo, hi):
        parts = [a[lo - f : hi - f] for f, t, a in received if f <= lo and hi <= t]
        total = parts[0]
        for part in parts[1:]:
            total = total + part
        return total

    def halve(at, lo, hi, to):
        got = swap_steps(summed(lo, hi), (at,), sizes)
        received.append((to, to + hi - lo, got))

    local(3 * q, q, away)
    halve(0, 3 * q, 4 * q, q)
    local(2 * q, q)
    halve(0, 2 * q, 3 * q, 0)
    local(q, q)
    halve(1, 3 * e, 4 * e, e)
    halve(1, 2 * e, 3 * e, 0)
    local(0, q)
    h = jnp.stack([data[2], data[3]]).astype(F32)
    h = h.transpose(2, 0, 1, 3).reshape(2 * DET, CH, bins)
    halve(2, e, 2 * e, 0)
    halve(3, e // 2, e, 0)
    last = summed(0, SUB)
    got = swap_steps(last, (4,), sizes)
    filters = solve(last, got)

    rest = (data[0], data[1], h, intersection.reshape(bins // LANES, LANES))
    near = [filters]
    for steps in ((3,), (2,), (2, 3)):
        near.append(swap_steps(filters, steps, sizes))
    near = jnp.concatenate(near, axis=0)
    quarters = [near]
    quarters.append(swap_steps(near, (1,), sizes))
    quarters.append(swap_steps(near, (0,), sizes))
    quarters.append(swap_steps(quarters[1], (0,), sizes))
    pieces, sums, places = [], [], []
    for n, mine in enumerate(quarters):
        other = swap_core(mine)
        for which, filt in enumerate((mine, other)):
            if (n, which) == (3, 1):
                real, imag, num = finish(
                    sizes, half, filt, rest, which, n * q, places, pieces, sums
                )
            else:
                piece, num = clean(sizes, half, filt, rest, which, n * q)
                pieces.append(piece)
                sums.append(num)
                places.append((which, n * q))
    totals = summed_over_bin(num, sizes)
    estimate = totals[:, 0] / jnp.sqrt(totals[:, 1])
    return (real, imag, estimate)


def solution(mesh):
    sizes = {"z": 8, "x": 4, "c": 2, "y": mesh.shape["bin"]}
    torus = Mesh(mesh.devices.reshape(*sizes.values()), tuple(sizes))
    in_specs = (
        P(SEG, None, "y"),
        P(SEG, None, "y"),
        P(SEG, None, "y"),
        P(SEG, None, "y"),
        P(SEG),
        P("y"),
    )
    out_specs = (P(SEG, "y"), P(SEG, "y"), P(SEG))

    def body(*args):
        return on_device(sizes, *args)

    return jax.shard_map(
        body, mesh=torus, in_specs=in_specs, out_specs=out_specs, check_vma=False
    )
```

```python
import jax
import jax.numpy as jnp
from jax import lax
from jax.experimental import pallas as pl
from jax.experimental.pallas import tpu as pltpu
from jax.sharding import Mesh
from jax.sharding import PartitionSpec as P


SEG = ("z", "x", "c")
LANES = 128
CH = 8
DET = 2
ROWS = 96
WROWS = 32
VMEM = pltpu.VMEM
F32 = jnp.float32


def gray(i):
    return i ^ (i >> 1)


def label(axis, i):
    return (gray(i >> 1) << 1) | (i & 1) if axis == "z" else gray(i)


def flip_pairs(axis, size, shift, bits):
    where = {label(axis, (i - shift) % size): i for i in range(size)}
    return [(i, where[label(axis, (i - shift) % size) ^ bits]) for i in range(size)]


STEPS = (
    (("x", 0, 0), ("x", 0, 1), ("z", 0, 0), ("z", 0, 1), ("z", 0, 2)),
    (("x", 0, 1), ("x", 0, 0), ("z", 2, 0), ("z", 2, 1), ("z", 2, 2)),
)
SUB = 2


def swap_steps(value, steps, sizes):
    nz, nx, nc = sizes["z"], sizes["x"], sizes["c"]
    pairs = []
    for z in range(nz):
        for x in range(nx):
            for c in range(nc):
                where = {"z": z, "x": x}
                for at in steps:
                    axis, shift, bit = STEPS[c][at]
                    where[axis] = dict(flip_pairs(axis, sizes[axis], shift, 1 << bit))[where[axis]]
                pairs.append(((z * nx + x) * nc + c, (where["z"] * nx + where["x"]) * nc + c))
    return lax.ppermute(value, SEG, pairs)


def swap_core(value):
    return lax.ppermute(value, "c", [(0, 1), (1, 0)])


def step_code(core, sizes):
    code = jnp.int32(0)
    for axis, shift, bit in STEPS[core][:-1]:
        ring = (lax.axis_index(axis) + (sizes[axis] - shift)) & (sizes[axis] - 1)
        code = code * 2 + ((label(axis, ring) >> bit) & 1)
    return code * SUB


def half_codes(sizes, half):
    core = lax.axis_index("c")
    code_a, code_b = step_code(0, sizes), step_code(1, sizes)
    own = jnp.where(core == 0, code_a, code_b)
    other = jnp.where(core == 0, code_b, code_a)
    return ((core * half, own), ((1 - core) * half, other))


def sublane(shape=(CH, LANES)):
    return lax.broadcasted_iota(jnp.int32, shape, 0)


def down(v, k):
    return v if k == 0 else pltpu.roll(v, CH - k, 0)


def params():
    return pltpu.CompilerParams(vmem_limit_bytes=16 << 20)


def cost(blocks, flops):
    return pl.CostEstimate(flops=blocks * flops, bytes_accessed=0, transcendentals=0)


def block_of(codes, which, p):
    base, code = codes[which]
    return base + (p ^ code)


def lanes_of(block):
    return pl.ds(pl.multiple_of(block * LANES, LANES), LANES)


def spectra_block(at, keep, mr_ref, mi_ref, hr_ref, hi_ref, store):
    low = sublane() < 4
    acc = [jnp.zeros((CH, LANES), F32) for _ in range(12)]
    for s in range(CH):
        mr = mr_ref[s, :, at].astype(F32)
        mi = mi_ref[s, :, at].astype(F32)
        kr = mr * keep[s]
        ki = mi * keep[s]
        acc[0] = acc[0] + (kr * mr + ki * mi)
        for k in range(1, 4):
            rr = down(mr, k)
            ri = down(mi, k)
            acc[2 * k - 1] = acc[2 * k - 1] + (kr * rr + ki * ri)
            acc[2 * k] = acc[2 * k] + (ki * rr - kr * ri)
        rr = down(mr, 4)
        ri = down(mi, 4)
        acc[7] = acc[7] + (jnp.where(low, kr, ki) * rr + jnp.where(low, ki, -kr) * ri)
        hr = hr_ref[s, :, at].astype(F32)
        hi = hi_ref[s, :, at].astype(F32)
        for k in range(DET):
            br = jnp.broadcast_to(hr[k : k + 1], (CH, LANES))
            bi = jnp.broadcast_to(hi[k : k + 1], (CH, LANES))
            acc[8 + 2 * k] = acc[8 + 2 * k] + (kr * br + ki * bi)
            acc[9 + 2 * k] = acc[9 + 2 * k] + (ki * br - kr * bi)
    for r in range(12):
        store(r, acc[r])


def spectra_loop(codes, which, first, count, keep, data, out_ref):
    def step(p, carry):
        def store(r, tile):
            out_ref[p, CH * r : CH * (r + 1), :] = tile

        spectra_block(lanes_of(block_of(codes, which, first + p)), keep, *data, store)
        return carry

    lax.fori_loop(0, count, step, 0)


def front_body(sizes, half, first, count, valid_hbm, *refs):
    hbm, (out_ref, keep_ref, *local) = refs[:4], refs[4:10]
    keep_smem, keep_sem, sems = refs[10:]
    codes = half_codes(sizes, half)
    width = count * LANES
    npiece = hbm[0].shape[2] // width
    lead = block_of(codes, 1, first) // count
    keep_copy = pltpu.make_async_copy(valid_hbm, keep_smem, keep_sem)
    keep_copy.start()
    copies = []
    for n in range(npiece):
        at = pl.ds(pl.multiple_of((n ^ lead) * width, width), width)
        copies.append(
            [
                pltpu.make_async_copy(src.at[:, :, at], dst.at[:, :, at], sems.at[n, i])
                for i, (src, dst) in enumerate(zip(hbm, local))
            ]
        )
        for copy in copies[-1]:
            copy.start()
    keep_copy.wait()
    for copy in copies[0]:
        copy.wait()
    for s in range(CH):
        keep_ref[s] = jnp.full((CH, LANES), keep_smem[s].astype(F32))
    spectra_loop(codes, 1, first, count, keep_ref, local, out_ref)
    for piece in copies[1:]:
        for copy in piece:
            copy.wait()


def front(sizes, half, valid, data, first, count):
    npiece = data[0].shape[2] // (count * LANES)
    return pl.pallas_call(
        lambda *refs: front_body(sizes, half, first, count, *refs),
        out_shape=[
            jax.ShapeDtypeStruct((count, ROWS, LANES), F32),
            jax.ShapeDtypeStruct((CH, CH, LANES), F32),
        ]
        + [jax.ShapeDtypeStruct(d.shape, d.dtype) for d in data],
        in_specs=[pl.BlockSpec(memory_space=pltpu.MemorySpace.HBM)] * 5,
        out_specs=[pl.BlockSpec(memory_space=VMEM)] * 6,
        scratch_shapes=[
            pltpu.SMEM(valid.shape, valid.dtype),
            pltpu.SemaphoreType.DMA,
            pltpu.SemaphoreType.DMA((npiece, 4)),
        ],
        compiler_params=params(),
        cost_estimate=cost(count, 500000),
        name="front",
    )(*(pltpu.with_memory_space_constraint(a, pltpu.MemorySpace.HBM) for a in (valid, *data)))


def spectra_body(sizes, half, which, first, count, keep_ref, *refs):
    spectra_loop(half_codes(sizes, half), which, first, count, keep_ref, refs[:4], refs[4])


def spectra(sizes, half, keep, data, which, first, count):
    return pl.pallas_call(
        lambda *refs: spectra_body(sizes, half, which, first, count, *refs),
        out_shape=jax.ShapeDtypeStruct((count, ROWS, LANES), F32),
        in_specs=[pl.BlockSpec(memory_space=VMEM)] * 5,
        out_specs=pl.BlockSpec(memory_space=VMEM),
        compiler_params=params(),
        cost_estimate=cost(count, 500000),
        name="spectra",
    )(keep, *data)


def solve_block(rows):
    sub = sublane()
    low = sub < 4
    dr = [None] * CH
    di = [None] * CH
    dr[0] = rows[0] + 1.0
    di[0] = jnp.zeros_like(rows[0])
    for k in range(1, 4):
        dr[k], di[k] = rows[2 * k - 1], rows[2 * k]
        dr[CH - k] = pltpu.roll(rows[2 * k - 1], k, 0)
        di[CH - k] = -pltpu.roll(rows[2 * k], k, 0)
    half = rows[7]
    turned = pltpu.roll(half, 4, 0)
    dr[4] = jnp.where(low, half, turned)
    di[4] = jnp.where(low, -turned, half)
    cols_r, cols_i = [], []
    for j in range(CH):
        cr, ci = dr[j], di[j]
        for c in range(1, CH):
            cr = jnp.where(sub == c, dr[(j - c) % CH], cr)
            ci = jnp.where(sub == c, di[(j - c) % CH], ci)
        cols_r.append(cr)
        cols_i.append(ci)
    cols_r += [rows[8], rows[10]]
    cols_i += [rows[9], rows[11]]

    def row(v, j):
        return jnp.broadcast_to(v[j : j + 1], (CH, LANES))

    diag = jnp.ones((CH, LANES), F32)
    for j in range(CH):
        pivot = row(cols_r[j], j)
        diag = jnp.where(sub == j, pivot, diag)
        inv = 1.0 / pivot
        fr = jnp.where(sub == j, 0.0, cols_r[j] * inv)
        fi = jnp.where(sub == j, 0.0, cols_i[j] * inv)
        for k in range(j + 1, CH + DET):
            ar, ai = row(cols_r[k], j), row(cols_i[k], j)
            cols_r[k] = cols_r[k] - (fr * ar - fi * ai)
            cols_i[k] = cols_i[k] - (fr * ai + fi * ar)
    inv = 1.0 / diag
    return [cols_r[8] * inv, cols_i[8] * inv, cols_r[9] * inv, cols_i[9] * inv]


def added_body(starts, count, *refs):
    for u in range(count):
        for r in range(ROWS // CH):
            rows = pl.ds(CH * r, CH)
            total = refs[0][starts[0] + u, rows, :]
            for start, ref in zip(starts[1:], refs[1:-1]):
                total = total + ref[start + u, rows, :]
            refs[-1][u, rows, :] = total


def added(arrays, starts, count):
    return pl.pallas_call(
        lambda *refs: added_body(starts, count, *refs),
        out_shape=jax.ShapeDtypeStruct((count, ROWS, LANES), F32),
        in_specs=[pl.BlockSpec(memory_space=VMEM)] * len(arrays),
        out_specs=pl.BlockSpec(memory_space=VMEM),
        compiler_params=params(),
        cost_estimate=cost(count, 50000),
        name="added",
    )(*arrays)


def solve_body(a_ref, b_ref, out_ref):
    for u in range(SUB):
        rows = [
            a_ref[u, CH * r : CH * (r + 1), :] + b_ref[u, CH * r : CH * (r + 1), :]
            for r in range(12)
        ]
        for q, tile in enumerate(solve_block(rows)):
            out_ref[u, CH * q : CH * (q + 1), :] = tile


def solve(a, b):
    return pl.pallas_call(
        solve_body,
        out_shape=jax.ShapeDtypeStruct((SUB, WROWS, LANES), F32),
        in_specs=[pl.BlockSpec(memory_space=VMEM)] * 2,
        out_specs=pl.BlockSpec(memory_space=VMEM),
        compiler_params=params(),
        cost_estimate=cost(SUB, 5000000),
        name="solve",
    )(a, b)


def channel_sums(tiles):
    sub = sublane()
    half = sub < 4
    level = []
    for s in range(4):
        a, b = tiles[s], tiles[s + 4]
        level.append(jnp.where(half, a, b) + pltpu.roll(jnp.where(half, b, a), 4, 0))
    for bit in (2, 1):
        mask = (sub & bit) == 0
        nxt = []
        for s in range(bit):
            a, b = level[s], level[s + bit]
            nxt.append(jnp.where(mask, a + pltpu.roll(a, CH - bit, 0), b + pltpu.roll(b, bit, 0)))
        level = nxt
    return level[0]


def clean_block(block, w, mr_ref, mi_ref, h_ref, inter_ref):
    at = lanes_of(block)
    parts = [[] for _ in range(4)]
    for s in range(CH):
        mr = mr_ref[s, :, at].astype(F32)
        mi = mi_ref[s, :, at].astype(F32)
        for k in range(DET):
            wr, wi = w[2 * k], w[2 * k + 1]
            parts[2 * k].append(wr * mr + wi * mi)
            parts[2 * k + 1].append(wr * mi - wi * mr)
    g = [h_ref[q, :, at] - channel_sums(parts[q]) for q in range(4)]
    real = g[0] * g[2] + g[1] * g[3]
    imag = g[1] * g[2] - g[0] * g[3]
    weight = jnp.broadcast_to(inter_ref[pl.ds(block, 1), :], (CH, LANES))
    return real, imag, real * weight


def filter_tiles(w_ref, p):
    return [w_ref[p, CH * q : CH * (q + 1), :] for q in range(4)]


def clean_body(sizes, half, which, first, count, last, w_ref, *refs):
    data, sums, (out_ref, num_ref) = refs[:4], refs[4:-2], refs[-2:]
    codes = half_codes(sizes, half)

    def step(p, num):
        block = block_of(codes, which, first + p)
        real, imag, part = clean_block(block, filter_tiles(w_ref, p), *data)
        out_ref[p, 0:CH, :] = real
        out_ref[p, CH : 2 * CH, :] = imag
        return num + part

    num = lax.fori_loop(0, count, step, jnp.zeros((CH, LANES), F32))
    for sum_ref in sums:
        num = num + sum_ref[...]
    if last:
        weight = data[3][...]
        square = jnp.sum(weight * weight)
        lane = lax.broadcasted_iota(jnp.int32, (CH, LANES), 1)
        total = jnp.broadcast_to(jnp.sum(num, axis=1, keepdims=True), (CH, LANES))
        num = jnp.where(lane == 0, total, square)
    num_ref[...] = num


def clean(sizes, half, filters, rest, which, first, sums):
    count = filters.shape[0]
    last = which == 1 and first + count == half
    args = (filters, *rest, *sums)
    return pl.pallas_call(
        lambda *refs: clean_body(sizes, half, which, first, count, last, *refs),
        out_shape=[
            jax.ShapeDtypeStruct((count, 2 * CH, LANES), F32),
            jax.ShapeDtypeStruct((CH, LANES), F32),
        ],
        in_specs=[pl.BlockSpec(memory_space=VMEM)] * len(args),
        out_specs=[pl.BlockSpec(memory_space=VMEM)] * 2,
        compiler_params=params(),
        cost_estimate=cost(count, 300000),
        name="clean",
    )(*args)


def merge_body(sizes, half, places, *refs):
    real_ref, imag_ref = refs[-2:]
    codes = half_codes(sizes, half)
    for (which, first), done_ref in zip(places, refs):
        for p in range(done_ref.shape[0]):
            at = lanes_of(block_of(codes, which, first + p))
            real_ref[:, at] = done_ref[p, 0:CH, :]
            imag_ref[:, at] = done_ref[p, CH : 2 * CH, :]


def merge(sizes, half, places, pieces, bins):
    return pl.pallas_call(
        lambda *refs: merge_body(sizes, half, places, *refs),
        out_shape=[jax.ShapeDtypeStruct((CH, bins), F32)] * 2,
        in_specs=[pl.BlockSpec(memory_space=VMEM)] * len(pieces),
        out_specs=[pl.BlockSpec(memory_space=VMEM)] * 2,
        compiler_params=params(),
        cost_estimate=cost(len(pieces), 300000),
        name="merge",
    )(*pieces)


def summed_over_bin(value, sizes):
    got = [value]
    for bits in range(1, sizes["y"]):
        got.append(lax.ppermute(value, "y", flip_pairs("y", sizes["y"], 0, bits)))
    while len(got) > 1:
        got = [a + b for a, b in zip(got[::2], got[1::2])]
    return got[0]


def on_device(sizes, magnet_real, magnet_imag, detector_real, detector_imag, valid, intersection):
    bins = magnet_real.shape[2]
    half = bins // (LANES * sizes["c"])
    q = half // 4
    e = half // 8
    data = (magnet_real, magnet_imag, detector_real, detector_imag)

    away, keep, *data = front(sizes, half, valid, data, 3 * q, q)
    received = []

    def local(first, count, away=None):
        if away is None:
            away = spectra(sizes, half, keep, data, 1, first, count)
        away = swap_core(away)
        own = spectra(sizes, half, keep, data, 0, first, count)
        received.extend([(first, first + count, own), (first, first + count, away)])

    def summed(lo, hi, alone=False):
        if alone:
            parts = [(a, lo - f) for f, t, a in received if f <= lo and hi <= t]
            return added(*zip(*parts), hi - lo)
        parts = [a[lo - f : hi - f] for f, t, a in received if f <= lo and hi <= t]
        total = parts[0]
        for part in parts[1:]:
            total = total + part
        return total

    def halve(at, lo, hi, to):
        got = swap_steps(summed(lo, hi), (at,), sizes)
        received.append((to, to + hi - lo, got))

    local(3 * q, q, away)
    halve(0, 3 * q, 4 * q, q)
    local(2 * q, q)
    halve(0, 2 * q, 3 * q, 0)
    local(q, q)
    halve(1, 3 * e, 4 * e, e)
    halve(1, 2 * e, 3 * e, 0)
    local(0, q)
    h = jnp.stack([data[2], data[3]]).astype(F32)
    h = h.transpose(2, 0, 1, 3).reshape(2 * DET, CH, bins)
    direct = []
    for n, steps in ((2, (2,)), (3, (2, 3)), (1, (3,))):
        send = summed(n * SUB, (n + 1) * SUB, alone=n == 1)
        direct.append((0, SUB, swap_steps(send, steps, sizes)))
    received.extend(direct)
    last = summed(0, SUB)
    got = swap_steps(last, (4,), sizes)
    filters = solve(last, got)

    rest = (data[0], data[1], h, intersection.reshape(bins // LANES, LANES))
    near = [filters]
    for steps in ((3,), (2,), (2, 3)):
        near.append(swap_steps(filters, steps, sizes))
    near = jnp.concatenate(near, axis=0)
    quarters = [near]
    for steps in ((1,), (0,), (0, 1)):
        quarters.append(swap_steps(near, steps, sizes))
    pieces, sums, places = [], [], []
    for n, mine in enumerate(quarters):
        other = swap_core(mine)
        for which, filt in enumerate((mine, other)):
            final = (n, which) == (3, 1)
            piece, num = clean(sizes, half, filt, rest, which, n * q, sums if final else ())
            pieces.append(piece)
            sums.append(num)
            places.append((which, n * q))
    real, imag = merge(sizes, half, places, pieces, bins)
    totals = summed_over_bin(num, sizes)
    estimate = totals[:, 0] / jnp.sqrt(totals[:, 1])
    return (real, imag, estimate)


def solution(mesh):
    sizes = {"z": 8, "x": 4, "c": 2, "y": mesh.shape["bin"]}
    torus = Mesh(mesh.devices.reshape(*sizes.values()), tuple(sizes))
    in_specs = (
        P(SEG, None, "y"),
        P(SEG, None, "y"),
        P(SEG, None, "y"),
        P(SEG, None, "y"),
        P(SEG),
        P("y"),
    )
    out_specs = (P(SEG, "y"), P(SEG, "y"), P(SEG))

    def body(*args):
        return on_device(sizes, *args)

    return jax.shard_map(
        body, mesh=torus, in_specs=in_specs, out_specs=out_specs, check_vma=False
    )
```

```python
import jax
import jax.numpy as jnp
from jax import lax
from jax.experimental import pallas as pl
from jax.experimental.pallas import tpu as pltpu
from jax.sharding import Mesh
from jax.sharding import PartitionSpec as P


SEG = ("z", "x", "c")
LANES = 128
CH = 8
DET = 2
ROWS = 96
WROWS = 32
VMEM = pltpu.VMEM
F32 = jnp.float32


def gray(i):
    return i ^ (i >> 1)


def label(axis, i):
    return (gray(i >> 1) << 1) | (i & 1) if axis == "z" else gray(i)


def flip_pairs(axis, size, shift, bits):
    where = {label(axis, (i - shift) % size): i for i in range(size)}
    return [(i, where[label(axis, (i - shift) % size) ^ bits]) for i in range(size)]


STEPS = (
    (("x", 0, 0), ("x", 0, 1), ("z", 0, 0), ("z", 0, 1), ("z", 0, 2)),
    (("x", 0, 1), ("x", 0, 0), ("z", 2, 0), ("z", 2, 1), ("z", 2, 2)),
)
SUB = 2


def swap_steps(value, steps, sizes):
    nz, nx, nc = sizes["z"], sizes["x"], sizes["c"]
    pairs = []
    for z in range(nz):
        for x in range(nx):
            for c in range(nc):
                where = {"z": z, "x": x}
                for at in steps:
                    axis, shift, bit = STEPS[c][at]
                    where[axis] = dict(flip_pairs(axis, sizes[axis], shift, 1 << bit))[where[axis]]
                pairs.append(((z * nx + x) * nc + c, (where["z"] * nx + where["x"]) * nc + c))
    return lax.ppermute(value, SEG, pairs)


def swap_core(value):
    return lax.ppermute(value, "c", [(0, 1), (1, 0)])


def step_code(core, sizes):
    code = jnp.int32(0)
    for axis, shift, bit in STEPS[core][:-1]:
        ring = (lax.axis_index(axis) + (sizes[axis] - shift)) & (sizes[axis] - 1)
        code = code * 2 + ((label(axis, ring) >> bit) & 1)
    return code * SUB


def half_codes(sizes, half):
    core = lax.axis_index("c")
    code_a, code_b = step_code(0, sizes), step_code(1, sizes)
    own = jnp.where(core == 0, code_a, code_b)
    other = jnp.where(core == 0, code_b, code_a)
    return ((core * half, own), ((1 - core) * half, other))


def sublane(shape=(CH, LANES)):
    return lax.broadcasted_iota(jnp.int32, shape, 0)


def down(v, k):
    return v if k == 0 else pltpu.roll(v, CH - k, 0)


def params():
    return pltpu.CompilerParams(vmem_limit_bytes=16 << 20)


def cost(blocks, flops):
    return pl.CostEstimate(flops=blocks * flops, bytes_accessed=0, transcendentals=0)


def block_of(codes, which, p):
    base, code = codes[which]
    return base + (p ^ code)


def lanes_of(block):
    return pl.ds(pl.multiple_of(block * LANES, LANES), LANES)


def spectra_block(at, keep, mr_ref, mi_ref, hr_ref, hi_ref, store):
    low = sublane() < 4
    acc = [jnp.zeros((CH, LANES), F32) for _ in range(12)]
    for s in range(CH):
        mr = mr_ref[s, :, at].astype(F32)
        mi = mi_ref[s, :, at].astype(F32)
        kr = mr * keep[s]
        ki = mi * keep[s]
        acc[0] = acc[0] + (kr * mr + ki * mi)
        for k in range(1, 4):
            rr = down(mr, k)
            ri = down(mi, k)
            acc[2 * k - 1] = acc[2 * k - 1] + (kr * rr + ki * ri)
            acc[2 * k] = acc[2 * k] + (ki * rr - kr * ri)
        rr = down(mr, 4)
        ri = down(mi, 4)
        acc[7] = acc[7] + (jnp.where(low, kr, ki) * rr + jnp.where(low, ki, -kr) * ri)
        hr = hr_ref[s, :, at].astype(F32)
        hi = hi_ref[s, :, at].astype(F32)
        for k in range(DET):
            br = jnp.broadcast_to(hr[k : k + 1], (CH, LANES))
            bi = jnp.broadcast_to(hi[k : k + 1], (CH, LANES))
            acc[8 + 2 * k] = acc[8 + 2 * k] + (kr * br + ki * bi)
            acc[9 + 2 * k] = acc[9 + 2 * k] + (ki * br - kr * bi)
    for r in range(12):
        store(r, acc[r])


def spectra_loop(codes, which, first, count, keep, data, out_ref):
    def step(p, carry):
        def store(r, tile):
            out_ref[p, CH * r : CH * (r + 1), :] = tile

        spectra_block(lanes_of(block_of(codes, which, first + p)), keep, *data, store)
        return carry

    lax.fori_loop(0, count, step, 0)


def front_body(sizes, half, first, count, valid_hbm, *refs):
    hbm, (out_ref, keep_ref, *local) = refs[:4], refs[4:10]
    keep_smem, keep_sem, sems = refs[10:]
    codes = half_codes(sizes, half)
    width = count * LANES
    npiece = hbm[0].shape[2] // width
    lead = block_of(codes, 1, first) // count
    keep_copy = pltpu.make_async_copy(valid_hbm, keep_smem, keep_sem)
    keep_copy.start()
    copies = []
    for n in range(npiece):
        at = pl.ds(pl.multiple_of((n ^ lead) * width, width), width)
        copies.append(
            [
                pltpu.make_async_copy(src.at[:, :, at], dst.at[:, :, at], sems.at[n, i])
                for i, (src, dst) in enumerate(zip(hbm, local))
            ]
        )
        for copy in copies[-1]:
            copy.start()
    keep_copy.wait()
    for copy in copies[0]:
        copy.wait()
    for s in range(CH):
        keep_ref[s] = jnp.full((CH, LANES), keep_smem[s].astype(F32))
    spectra_loop(codes, 1, first, count, keep_ref, local, out_ref)
    for piece in copies[1:]:
        for copy in piece:
            copy.wait()


def front(sizes, half, valid, data, first, count):
    npiece = data[0].shape[2] // (count * LANES)
    return pl.pallas_call(
        lambda *refs: front_body(sizes, half, first, count, *refs),
        out_shape=[
            jax.ShapeDtypeStruct((count, ROWS, LANES), F32),
            jax.ShapeDtypeStruct((CH, CH, LANES), F32),
        ]
        + [jax.ShapeDtypeStruct(d.shape, d.dtype) for d in data],
        in_specs=[pl.BlockSpec(memory_space=pltpu.MemorySpace.HBM)] * 5,
        out_specs=[pl.BlockSpec(memory_space=VMEM)] * 6,
        scratch_shapes=[
            pltpu.SMEM(valid.shape, valid.dtype),
            pltpu.SemaphoreType.DMA,
            pltpu.SemaphoreType.DMA((npiece, 4)),
        ],
        compiler_params=params(),
        cost_estimate=cost(count, 500000),
        name="front",
    )(*(pltpu.with_memory_space_constraint(a, pltpu.MemorySpace.HBM) for a in (valid, *data)))


def spectra_body(sizes, half, which, first, count, keep_ref, *refs):
    spectra_loop(half_codes(sizes, half), which, first, count, keep_ref, refs[:4], refs[4])


def spectra(sizes, half, keep, data, which, first, count):
    return pl.pallas_call(
        lambda *refs: spectra_body(sizes, half, which, first, count, *refs),
        out_shape=jax.ShapeDtypeStruct((count, ROWS, LANES), F32),
        in_specs=[pl.BlockSpec(memory_space=VMEM)] * 5,
        out_specs=pl.BlockSpec(memory_space=VMEM),
        compiler_params=params(),
        cost_estimate=cost(count, 500000),
        name="spectra",
    )(keep, *data)


def solve_block(rows):
    sub = sublane()
    low = sub < 4
    dr = [None] * CH
    di = [None] * CH
    dr[0] = rows[0] + 1.0
    di[0] = jnp.zeros_like(rows[0])
    for k in range(1, 4):
        dr[k], di[k] = rows[2 * k - 1], rows[2 * k]
        dr[CH - k] = pltpu.roll(rows[2 * k - 1], k, 0)
        di[CH - k] = -pltpu.roll(rows[2 * k], k, 0)
    half = rows[7]
    turned = pltpu.roll(half, 4, 0)
    dr[4] = jnp.where(low, half, turned)
    di[4] = jnp.where(low, -turned, half)
    cols_r, cols_i = [], []
    for j in range(CH):
        cr, ci = dr[j], di[j]
        for c in range(1, CH):
            cr = jnp.where(sub == c, dr[(j - c) % CH], cr)
            ci = jnp.where(sub == c, di[(j - c) % CH], ci)
        cols_r.append(cr)
        cols_i.append(ci)
    cols_r += [rows[8], rows[10]]
    cols_i += [rows[9], rows[11]]

    def row(v, j):
        return jnp.broadcast_to(v[j : j + 1], (CH, LANES))

    diag = jnp.ones((CH, LANES), F32)
    for j in range(CH):
        pivot = row(cols_r[j], j)
        diag = jnp.where(sub == j, pivot, diag)
        inv = 1.0 / pivot
        fr = jnp.where(sub == j, 0.0, cols_r[j] * inv)
        fi = jnp.where(sub == j, 0.0, cols_i[j] * inv)
        for k in range(j + 1, CH + DET):
            ar, ai = row(cols_r[k], j), row(cols_i[k], j)
            cols_r[k] = cols_r[k] - (fr * ar - fi * ai)
            cols_i[k] = cols_i[k] - (fr * ai + fi * ar)
    inv = 1.0 / diag
    return [cols_r[8] * inv, cols_i[8] * inv, cols_r[9] * inv, cols_i[9] * inv]


def added_body(starts, count, *refs):
    for u in range(count):
        for r in range(ROWS // CH):
            rows = pl.ds(CH * r, CH)
            total = refs[0][starts[0] + u, rows, :]
            for start, ref in zip(starts[1:], refs[1:-1]):
                total = total + ref[start + u, rows, :]
            refs[-1][u, rows, :] = total


def added(arrays, starts, count):
    return pl.pallas_call(
        lambda *refs: added_body(starts, count, *refs),
        out_shape=jax.ShapeDtypeStruct((count, ROWS, LANES), F32),
        in_specs=[pl.BlockSpec(memory_space=VMEM)] * len(arrays),
        out_specs=pl.BlockSpec(memory_space=VMEM),
        compiler_params=params(),
        cost_estimate=cost(count, 50000),
        name="added",
    )(*arrays)


def solve_body(a_ref, b_ref, out_ref):
    for u in range(SUB):
        rows = [
            a_ref[u, CH * r : CH * (r + 1), :] + b_ref[u, CH * r : CH * (r + 1), :]
            for r in range(12)
        ]
        for q, tile in enumerate(solve_block(rows)):
            out_ref[u, CH * q : CH * (q + 1), :] = tile


def solve(a, b):
    return pl.pallas_call(
        solve_body,
        out_shape=jax.ShapeDtypeStruct((SUB, WROWS, LANES), F32),
        in_specs=[pl.BlockSpec(memory_space=VMEM)] * 2,
        out_specs=pl.BlockSpec(memory_space=VMEM),
        compiler_params=params(),
        cost_estimate=cost(SUB, 5000000),
        name="solve",
    )(a, b)


def channel_sums(tiles):
    sub = sublane()
    half = sub < 4
    level = []
    for s in range(4):
        a, b = tiles[s], tiles[s + 4]
        level.append(jnp.where(half, a, b) + pltpu.roll(jnp.where(half, b, a), 4, 0))
    for bit in (2, 1):
        mask = (sub & bit) == 0
        nxt = []
        for s in range(bit):
            a, b = level[s], level[s + bit]
            nxt.append(jnp.where(mask, a + pltpu.roll(a, CH - bit, 0), b + pltpu.roll(b, bit, 0)))
        level = nxt
    return level[0]


def clean_block(block, w, mr_ref, mi_ref, h_ref, inter_ref):
    at = lanes_of(block)
    parts = [[] for _ in range(4)]
    for s in range(CH):
        mr = mr_ref[s, :, at].astype(F32)
        mi = mi_ref[s, :, at].astype(F32)
        for k in range(DET):
            wr, wi = w[2 * k], w[2 * k + 1]
            parts[2 * k].append(wr * mr + wi * mi)
            parts[2 * k + 1].append(wr * mi - wi * mr)
    g = [h_ref[q, :, at] - channel_sums(parts[q]) for q in range(4)]
    real = g[0] * g[2] + g[1] * g[3]
    imag = g[1] * g[2] - g[0] * g[3]
    weight = jnp.broadcast_to(inter_ref[pl.ds(block, 1), :], (CH, LANES))
    return real, imag, real * weight


def filter_tiles(w_ref, p):
    return [w_ref[p, CH * q : CH * (q + 1), :] for q in range(4)]


def clean_body(sizes, half, which, first, count, last, w_ref, *refs):
    data, sums, (out_ref, num_ref) = refs[:4], refs[4:-2], refs[-2:]
    codes = half_codes(sizes, half)

    def step(p, num):
        block = block_of(codes, which, first + p)
        real, imag, part = clean_block(block, filter_tiles(w_ref, p), *data)
        out_ref[p, 0:CH, :] = real
        out_ref[p, CH : 2 * CH, :] = imag
        return num + part

    num = lax.fori_loop(0, count, step, jnp.zeros((CH, LANES), F32))
    for sum_ref in sums:
        num = num + sum_ref[...]
    if last:
        weight = data[3][...]
        square = jnp.sum(weight * weight)
        lane = lax.broadcasted_iota(jnp.int32, (CH, LANES), 1)
        total = jnp.broadcast_to(jnp.sum(num, axis=1, keepdims=True), (CH, LANES))
        total = jnp.sum(jnp.where(lane == sublane(), total, 0.0), axis=0, keepdims=True)
        num = jnp.where(sublane() == 0, jnp.broadcast_to(total, (CH, LANES)), square)
    num_ref[...] = num


def clean(sizes, half, filters, rest, which, first, sums):
    count = filters.shape[0]
    last = which == 1 and first + count == half
    args = (filters, *rest, *sums)
    return pl.pallas_call(
        lambda *refs: clean_body(sizes, half, which, first, count, last, *refs),
        out_shape=[
            jax.ShapeDtypeStruct((count, 2 * CH, LANES), F32),
            jax.ShapeDtypeStruct((CH, LANES), F32),
        ],
        in_specs=[pl.BlockSpec(memory_space=VMEM)] * len(args),
        out_specs=[pl.BlockSpec(memory_space=VMEM)] * 2,
        compiler_params=params(),
        cost_estimate=cost(count, 300000),
        name="clean",
    )(*args)


def merge_body(sizes, half, places, *refs):
    real_ref, imag_ref = refs[-2:]
    codes = half_codes(sizes, half)
    for (which, first), done_ref in zip(places, refs):
        for p in range(done_ref.shape[0]):
            at = lanes_of(block_of(codes, which, first + p))
            real_ref[:, at] = done_ref[p, 0:CH, :]
            imag_ref[:, at] = done_ref[p, CH : 2 * CH, :]


def merge(sizes, half, places, pieces, bins):
    return pl.pallas_call(
        lambda *refs: merge_body(sizes, half, places, *refs),
        out_shape=[jax.ShapeDtypeStruct((CH, bins), F32)] * 2,
        in_specs=[pl.BlockSpec(memory_space=VMEM)] * len(pieces),
        out_specs=[pl.BlockSpec(memory_space=VMEM)] * 2,
        compiler_params=params(),
        cost_estimate=cost(len(pieces), 300000),
        name="merge",
    )(*pieces)


def summed_over_bin(value, sizes):
    got = [value]
    for bits in range(1, sizes["y"]):
        got.append(lax.ppermute(value, "y", flip_pairs("y", sizes["y"], 0, bits)))
    while len(got) > 1:
        got = [a + b for a, b in zip(got[::2], got[1::2])]
    return got[0]


def on_device(sizes, magnet_real, magnet_imag, detector_real, detector_imag, valid, intersection):
    bins = magnet_real.shape[2]
    half = bins // (LANES * sizes["c"])
    q = half // 4
    e = half // 8
    data = (magnet_real, magnet_imag, detector_real, detector_imag)

    away, keep, *data = front(sizes, half, valid, data, 3 * q, q)
    received = []

    def local(first, count, away=None):
        if away is None:
            away = spectra(sizes, half, keep, data, 1, first, count)
        away = swap_core(away)
        own = spectra(sizes, half, keep, data, 0, first, count)
        received.extend([(first, first + count, own), (first, first + count, away)])

    def summed(lo, hi, alone=False):
        if alone:
            parts = [(a, lo - f) for f, t, a in received if f <= lo and hi <= t]
            return added(*zip(*parts), hi - lo)
        parts = [a[lo - f : hi - f] for f, t, a in received if f <= lo and hi <= t]
        total = parts[0]
        for part in parts[1:]:
            total = total + part
        return total

    def halve(at, lo, hi, to):
        got = swap_steps(summed(lo, hi), (at,), sizes)
        received.append((to, to + hi - lo, got))

    local(3 * q, q, away)
    halve(0, 3 * q, 4 * q, q)
    local(2 * q, q)
    halve(0, 2 * q, 3 * q, 0)
    local(q, q)
    halve(1, 3 * e, 4 * e, e)
    halve(1, 2 * e, 3 * e, 0)
    local(0, q)
    h = jnp.stack([data[2], data[3]]).astype(F32)
    h = h.transpose(2, 0, 1, 3).reshape(2 * DET, CH, bins)
    direct = []
    for n, steps in ((2, (2,)), (3, (2, 3)), (1, (3,))):
        send = summed(n * SUB, (n + 1) * SUB, alone=n == 1)
        direct.append((0, SUB, swap_steps(send, steps, sizes)))
    received.extend(direct)
    last = summed(0, SUB)
    got = swap_steps(last, (4,), sizes)
    filters = solve(last, got)

    rest = (data[0], data[1], h, intersection.reshape(bins // LANES, LANES))
    near = [filters]
    for steps in ((3,), (2,), (2, 3)):
        near.append(swap_steps(filters, steps, sizes))
    near = jnp.concatenate(near, axis=0)
    quarters = [near]
    for steps in ((1,), (0,), (0, 1)):
        quarters.append(swap_steps(near, steps, sizes))
    pieces, sums, places = [], [], []
    for n, mine in enumerate(quarters):
        other = swap_core(mine)
        for which, filt in enumerate((mine, other)):
            final = (n, which) == (3, 1)
            piece, num = clean(sizes, half, filt, rest, which, n * q, sums if final else ())
            pieces.append(piece)
            sums.append(num)
            places.append((which, n * q))
    real, imag = merge(sizes, half, places, pieces, bins)
    totals = summed_over_bin(num, sizes)
    estimate = (totals[0] / jnp.sqrt(totals[1]))[:CH]
    return (real, imag, estimate)


def solution(mesh):
    sizes = {"z": 8, "x": 4, "c": 2, "y": mesh.shape["bin"]}
    torus = Mesh(mesh.devices.reshape(*sizes.values()), tuple(sizes))
    in_specs = (
        P(SEG, None, "y"),
        P(SEG, None, "y"),
        P(SEG, None, "y"),
        P(SEG, None, "y"),
        P(SEG),
        P("y"),
    )
    out_specs = (P(SEG, "y"), P(SEG, "y"), P(SEG))

    def body(*args):
        return on_device(sizes, *args)

    return jax.shard_map(
        body, mesh=torus, in_specs=in_specs, out_specs=out_specs, check_vma=False
    )
```

```python
import jax
import jax.numpy as jnp
from jax import lax
from jax.experimental import pallas as pl
from jax.experimental.pallas import tpu as pltpu
from jax.sharding import Mesh
from jax.sharding import PartitionSpec as P


SEG = ("z", "x", "c")
LANES = 128
CH = 8
DET = 2
ROWS = 96
WROWS = 32
VMEM = pltpu.VMEM
F32 = jnp.float32


def gray(i):
    return i ^ (i >> 1)


def label(axis, i):
    return (gray(i >> 1) << 1) | (i & 1) if axis == "z" else gray(i)


def flip_pairs(axis, size, shift, bits):
    where = {label(axis, (i - shift) % size): i for i in range(size)}
    return [(i, where[label(axis, (i - shift) % size) ^ bits]) for i in range(size)]


STEPS = (
    (("x", 0, 0), ("x", 0, 1), ("z", 0, 0), ("z", 0, 1), ("z", 0, 2)),
    (("x", 0, 1), ("x", 0, 0), ("z", 2, 0), ("z", 2, 1), ("z", 2, 2)),
)
SUB = 2


def swap_steps(value, steps, sizes):
    nz, nx, nc = sizes["z"], sizes["x"], sizes["c"]
    pairs = []
    for z in range(nz):
        for x in range(nx):
            for c in range(nc):
                where = {"z": z, "x": x}
                for at in steps:
                    axis, shift, bit = STEPS[c][at]
                    where[axis] = dict(flip_pairs(axis, sizes[axis], shift, 1 << bit))[where[axis]]
                pairs.append(((z * nx + x) * nc + c, (where["z"] * nx + where["x"]) * nc + c))
    return lax.ppermute(value, SEG, pairs)


def swap_core(value):
    return lax.ppermute(value, "c", [(0, 1), (1, 0)])


def step_code(core, sizes):
    code = jnp.int32(0)
    for axis, shift, bit in STEPS[core][:-1]:
        ring = (lax.axis_index(axis) + (sizes[axis] - shift)) & (sizes[axis] - 1)
        code = code * 2 + ((label(axis, ring) >> bit) & 1)
    return code * SUB


def half_codes(sizes, half):
    core = lax.axis_index("c")
    code_a, code_b = step_code(0, sizes), step_code(1, sizes)
    own = jnp.where(core == 0, code_a, code_b)
    other = jnp.where(core == 0, code_b, code_a)
    return ((core * half, own), ((1 - core) * half, other))


def sublane(shape=(CH, LANES)):
    return lax.broadcasted_iota(jnp.int32, shape, 0)


def down(v, k):
    return v if k == 0 else pltpu.roll(v, CH - k, 0)


def params():
    return pltpu.CompilerParams(vmem_limit_bytes=16 << 20)


def cost(blocks, flops):
    return pl.CostEstimate(flops=blocks * flops, bytes_accessed=0, transcendentals=0)


def block_of(codes, which, p):
    base, code = codes[which]
    return base + (p ^ code)


def lanes_of(block):
    return pl.ds(pl.multiple_of(block * LANES, LANES), LANES)


def spectra_block(at, keep, mr_ref, mi_ref, hr_ref, hi_ref, store):
    low = sublane() < 4
    acc = [jnp.zeros((CH, LANES), F32) for _ in range(12)]
    for s in range(CH):
        mr = mr_ref[s, :, at].astype(F32)
        mi = mi_ref[s, :, at].astype(F32)
        kr = mr * keep[s]
        ki = mi * keep[s]
        acc[0] = acc[0] + (kr * mr + ki * mi)
        for k in range(1, 4):
            rr = down(mr, k)
            ri = down(mi, k)
            acc[2 * k - 1] = acc[2 * k - 1] + (kr * rr + ki * ri)
            acc[2 * k] = acc[2 * k] + (ki * rr - kr * ri)
        rr = down(mr, 4)
        ri = down(mi, 4)
        acc[7] = acc[7] + (jnp.where(low, kr, ki) * rr + jnp.where(low, ki, -kr) * ri)
        hr = hr_ref[s, :, at].astype(F32)
        hi = hi_ref[s, :, at].astype(F32)
        for k in range(DET):
            br = jnp.broadcast_to(hr[k : k + 1], (CH, LANES))
            bi = jnp.broadcast_to(hi[k : k + 1], (CH, LANES))
            acc[8 + 2 * k] = acc[8 + 2 * k] + (kr * br + ki * bi)
            acc[9 + 2 * k] = acc[9 + 2 * k] + (ki * br - kr * bi)
    for r in range(12):
        store(r, acc[r])


def spectra_loop(codes, which, first, count, keep, data, out_ref):
    def step(p, carry):
        def store(r, tile):
            out_ref[p, CH * r : CH * (r + 1), :] = tile

        spectra_block(lanes_of(block_of(codes, which, first + p)), keep, *data, store)
        return carry

    lax.fori_loop(0, count, step, 0)


def front_body(sizes, half, first, count, valid_hbm, *refs):
    hbm, (out_ref, keep_ref, *local) = refs[:4], refs[4:10]
    keep_smem, keep_sem, sems = refs[10:]
    codes = half_codes(sizes, half)
    width = count * LANES
    npiece = hbm[0].shape[2] // width
    lead = block_of(codes, 1, first) // count
    keep_copy = pltpu.make_async_copy(valid_hbm, keep_smem, keep_sem)
    keep_copy.start()
    copies = []
    for n in range(npiece):
        at = pl.ds(pl.multiple_of((n ^ lead) * width, width), width)
        copies.append(
            [
                pltpu.make_async_copy(src.at[:, :, at], dst.at[:, :, at], sems.at[n, i])
                for i, (src, dst) in enumerate(zip(hbm, local))
            ]
        )
        for copy in copies[-1]:
            copy.start()
    keep_copy.wait()
    for copy in copies[0]:
        copy.wait()
    for s in range(CH):
        keep_ref[s] = jnp.full((CH, LANES), keep_smem[s].astype(F32))
    spectra_loop(codes, 1, first, count, keep_ref, local, out_ref)
    for piece in copies[1:]:
        for copy in piece:
            copy.wait()


def front(sizes, half, valid, data, first, count):
    npiece = data[0].shape[2] // (count * LANES)
    return pl.pallas_call(
        lambda *refs: front_body(sizes, half, first, count, *refs),
        out_shape=[
            jax.ShapeDtypeStruct((count, ROWS, LANES), F32),
            jax.ShapeDtypeStruct((CH, CH, LANES), F32),
        ]
        + [jax.ShapeDtypeStruct(d.shape, d.dtype) for d in data],
        in_specs=[pl.BlockSpec(memory_space=pltpu.MemorySpace.HBM)] * 5,
        out_specs=[pl.BlockSpec(memory_space=VMEM)] * 6,
        scratch_shapes=[
            pltpu.SMEM(valid.shape, valid.dtype),
            pltpu.SemaphoreType.DMA,
            pltpu.SemaphoreType.DMA((npiece, 4)),
        ],
        compiler_params=params(),
        cost_estimate=cost(count, 500000),
        name="front",
    )(*(pltpu.with_memory_space_constraint(a, pltpu.MemorySpace.HBM) for a in (valid, *data)))


def spectra_body(sizes, half, which, first, count, keep_ref, *refs):
    spectra_loop(half_codes(sizes, half), which, first, count, keep_ref, refs[:4], refs[4])


def spectra(sizes, half, keep, data, which, first, count):
    return pl.pallas_call(
        lambda *refs: spectra_body(sizes, half, which, first, count, *refs),
        out_shape=jax.ShapeDtypeStruct((count, ROWS, LANES), F32),
        in_specs=[pl.BlockSpec(memory_space=VMEM)] * 5,
        out_specs=pl.BlockSpec(memory_space=VMEM),
        compiler_params=params(),
        cost_estimate=cost(count, 500000),
        name="spectra",
    )(keep, *data)


def solve_block(rows):
    sub = sublane()
    low = sub < 4
    dr = [None] * CH
    di = [None] * CH
    dr[0] = rows[0] + 1.0
    di[0] = jnp.zeros_like(rows[0])
    for k in range(1, 4):
        dr[k], di[k] = rows[2 * k - 1], rows[2 * k]
        dr[CH - k] = pltpu.roll(rows[2 * k - 1], k, 0)
        di[CH - k] = -pltpu.roll(rows[2 * k], k, 0)
    half = rows[7]
    turned = pltpu.roll(half, 4, 0)
    dr[4] = jnp.where(low, half, turned)
    di[4] = jnp.where(low, -turned, half)
    cols_r, cols_i = [], []
    for j in range(CH):
        cr, ci = dr[j], di[j]
        for c in range(1, CH):
            cr = jnp.where(sub == c, dr[(j - c) % CH], cr)
            ci = jnp.where(sub == c, di[(j - c) % CH], ci)
        cols_r.append(cr)
        cols_i.append(ci)
    cols_r += [rows[8], rows[10]]
    cols_i += [rows[9], rows[11]]

    def row(v, j):
        return jnp.broadcast_to(v[j : j + 1], (CH, LANES))

    diag = jnp.ones((CH, LANES), F32)
    for j in range(CH):
        pivot = row(cols_r[j], j)
        diag = jnp.where(sub == j, pivot, diag)
        inv = 1.0 / pivot
        fr = jnp.where(sub == j, 0.0, cols_r[j] * inv)
        fi = jnp.where(sub == j, 0.0, cols_i[j] * inv)
        for k in range(j + 1, CH + DET):
            ar, ai = row(cols_r[k], j), row(cols_i[k], j)
            cols_r[k] = cols_r[k] - (fr * ar - fi * ai)
            cols_i[k] = cols_i[k] - (fr * ai + fi * ar)
    inv = 1.0 / diag
    return [cols_r[8] * inv, cols_i[8] * inv, cols_r[9] * inv, cols_i[9] * inv]


def added_body(starts, count, *refs):
    for u in range(count):
        for r in range(ROWS // CH):
            rows = pl.ds(CH * r, CH)
            total = refs[0][starts[0] + u, rows, :]
            for start, ref in zip(starts[1:], refs[1:-1]):
                total = total + ref[start + u, rows, :]
            refs[-1][u, rows, :] = total


def added(arrays, starts, count):
    return pl.pallas_call(
        lambda *refs: added_body(starts, count, *refs),
        out_shape=jax.ShapeDtypeStruct((count, ROWS, LANES), F32),
        in_specs=[pl.BlockSpec(memory_space=VMEM)] * len(arrays),
        out_specs=pl.BlockSpec(memory_space=VMEM),
        compiler_params=params(),
        cost_estimate=cost(count, 50000),
        name="added",
    )(*arrays)


def solve_body(a_ref, b_ref, out_ref):
    for u in range(SUB):
        rows = [
            a_ref[u, CH * r : CH * (r + 1), :] + b_ref[u, CH * r : CH * (r + 1), :]
            for r in range(12)
        ]
        for q, tile in enumerate(solve_block(rows)):
            out_ref[u, CH * q : CH * (q + 1), :] = tile


def solve(a, b):
    return pl.pallas_call(
        solve_body,
        out_shape=jax.ShapeDtypeStruct((SUB, WROWS, LANES), F32),
        in_specs=[pl.BlockSpec(memory_space=VMEM)] * 2,
        out_specs=pl.BlockSpec(memory_space=VMEM),
        compiler_params=params(),
        cost_estimate=cost(SUB, 5000000),
        name="solve",
    )(a, b)


def channel_sums(tiles):
    sub = sublane()
    half = sub < 4
    level = []
    for s in range(4):
        a, b = tiles[s], tiles[s + 4]
        level.append(jnp.where(half, a, b) + pltpu.roll(jnp.where(half, b, a), 4, 0))
    for bit in (2, 1):
        mask = (sub & bit) == 0
        nxt = []
        for s in range(bit):
            a, b = level[s], level[s + bit]
            nxt.append(jnp.where(mask, a + pltpu.roll(a, CH - bit, 0), b + pltpu.roll(b, bit, 0)))
        level = nxt
    return level[0]


def clean_block(block, w, mr_ref, mi_ref, h_ref, inter_ref):
    at = lanes_of(block)
    parts = [[] for _ in range(4)]
    for s in range(CH):
        mr = mr_ref[s, :, at].astype(F32)
        mi = mi_ref[s, :, at].astype(F32)
        for k in range(DET):
            wr, wi = w[2 * k], w[2 * k + 1]
            parts[2 * k].append(wr * mr + wi * mi)
            parts[2 * k + 1].append(wr * mi - wi * mr)
    g = [h_ref[q, :, at] - channel_sums(parts[q]) for q in range(4)]
    real = g[0] * g[2] + g[1] * g[3]
    imag = g[1] * g[2] - g[0] * g[3]
    weight = jnp.broadcast_to(inter_ref[pl.ds(block, 1), :], (CH, LANES))
    return real, imag, real * weight


def filter_tiles(w_ref, p):
    return [w_ref[p, CH * q : CH * (q + 1), :] for q in range(4)]


def clean_body(sizes, half, which, first, count, last, w_ref, *refs):
    data, sums, (out_ref, num_ref) = refs[:4], refs[4:-2], refs[-2:]
    codes = half_codes(sizes, half)

    def step(p, num):
        block = block_of(codes, which, first + p)
        real, imag, part = clean_block(block, filter_tiles(w_ref, p), *data)
        out_ref[p, 0:CH, :] = real
        out_ref[p, CH : 2 * CH, :] = imag
        return num + part

    num = lax.fori_loop(0, count, step, jnp.zeros((CH, LANES), F32), unroll=2)
    for sum_ref in sums:
        num = num + sum_ref[...]
    if last:
        weight = data[3][...]
        square = jnp.sum(weight * weight)
        lane = lax.broadcasted_iota(jnp.int32, (CH, LANES), 1)
        total = jnp.broadcast_to(jnp.sum(num, axis=1, keepdims=True), (CH, LANES))
        total = jnp.sum(jnp.where(lane == sublane(), total, 0.0), axis=0, keepdims=True)
        num_ref[0:1, :] = total
        num_ref[1:2, :] = jnp.full((1, LANES), square)
    else:
        num_ref[...] = num


def clean(sizes, half, filters, rest, which, first, sums):
    count = filters.shape[0]
    last = which == 1 and first + count == half
    args = (filters, *rest, *sums)
    return pl.pallas_call(
        lambda *refs: clean_body(sizes, half, which, first, count, last, *refs),
        out_shape=[
            jax.ShapeDtypeStruct((count, 2 * CH, LANES), F32),
            jax.ShapeDtypeStruct((2 if last else CH, LANES), F32),
        ],
        in_specs=[pl.BlockSpec(memory_space=VMEM)] * len(args),
        out_specs=[pl.BlockSpec(memory_space=VMEM)] * 2,
        compiler_params=params(),
        cost_estimate=cost(count, 300000),
        name="clean",
    )(*args)


def merge_body(sizes, half, places, *refs):
    real_ref, imag_ref = refs[-2:]
    codes = half_codes(sizes, half)
    for (which, first), done_ref in zip(places, refs):
        for p in range(done_ref.shape[0]):
            at = lanes_of(block_of(codes, which, first + p))
            real_ref[:, at] = done_ref[p, 0:CH, :]
            imag_ref[:, at] = done_ref[p, CH : 2 * CH, :]


def merge(sizes, half, places, pieces, bins):
    return pl.pallas_call(
        lambda *refs: merge_body(sizes, half, places, *refs),
        out_shape=[jax.ShapeDtypeStruct((CH, bins), F32)] * 2,
        in_specs=[pl.BlockSpec(memory_space=VMEM)] * len(pieces),
        out_specs=[pl.BlockSpec(memory_space=VMEM)] * 2,
        compiler_params=params(),
        cost_estimate=cost(len(pieces), 300000),
        name="merge",
    )(*pieces)


def summed_over_bin(value, sizes):
    got = [value]
    for bits in range(1, sizes["y"]):
        got.append(lax.ppermute(value, "y", flip_pairs("y", sizes["y"], 0, bits)))
    while len(got) > 1:
        got = [a + b for a, b in zip(got[::2], got[1::2])]
    return got[0]


def on_device(sizes, magnet_real, magnet_imag, detector_real, detector_imag, valid, intersection):
    bins = magnet_real.shape[2]
    half = bins // (LANES * sizes["c"])
    q = half // 4
    e = half // 8
    data = (magnet_real, magnet_imag, detector_real, detector_imag)

    away, keep, *data = front(sizes, half, valid, data, 3 * q, q)
    received = []

    def local(first, count, away=None):
        if away is None:
            away = spectra(sizes, half, keep, data, 1, first, count)
        away = swap_core(away)
        own = spectra(sizes, half, keep, data, 0, first, count)
        received.extend([(first, first + count, own), (first, first + count, away)])

    def summed(lo, hi, alone=False):
        if alone:
            parts = [(a, lo - f) for f, t, a in received if f <= lo and hi <= t]
            return added(*zip(*parts), hi - lo)
        parts = [a[lo - f : hi - f] for f, t, a in received if f <= lo and hi <= t]
        total = parts[0]
        for part in parts[1:]:
            total = total + part
        return total

    def halve(at, lo, hi, to):
        got = swap_steps(summed(lo, hi), (at,), sizes)
        received.append((to, to + hi - lo, got))

    local(3 * q, q, away)
    halve(0, 3 * q, 4 * q, q)
    local(2 * q, q)
    halve(0, 2 * q, 3 * q, 0)
    local(q, q)
    halve(1, 3 * e, 4 * e, e)
    halve(1, 2 * e, 3 * e, 0)
    local(0, q)
    h = jnp.stack([data[2], data[3]]).astype(F32)
    h = h.transpose(2, 0, 1, 3).reshape(2 * DET, CH, bins)
    direct = []
    for n, steps in ((2, (2,)), (3, (2, 3)), (1, (3,))):
        send = summed(n * SUB, (n + 1) * SUB, alone=n == 1)
        direct.append((0, SUB, swap_steps(send, steps, sizes)))
    received.extend(direct)
    last = summed(0, SUB)
    got = swap_steps(last, (4,), sizes)
    filters = solve(last, got)

    rest = (data[0], data[1], h, intersection.reshape(bins // LANES, LANES))
    near = [filters]
    for steps in ((3,), (2,), (2, 3)):
        near.append(swap_steps(filters, steps, sizes))
    near = jnp.concatenate(near, axis=0)
    quarters = [near]
    for steps in ((1,), (0,), (0, 1)):
        quarters.append(swap_steps(near, steps, sizes))
    pieces, sums, places = [], [], []
    for n, mine in enumerate(quarters):
        other = swap_core(mine)
        for which, filt in enumerate((mine, other)):
            final = (n, which) == (3, 1)
            piece, num = clean(sizes, half, filt, rest, which, n * q, sums if final else ())
            pieces.append(piece)
            sums.append(num)
            places.append((which, n * q))
    real, imag = merge(sizes, half, places, pieces, bins)
    totals = summed_over_bin(num, sizes)
    estimate = (totals[0] / jnp.sqrt(totals[1]))[:CH]
    return (real, imag, estimate)


def solution(mesh):
    sizes = {"z": 8, "x": 4, "c": 2, "y": mesh.shape["bin"]}
    torus = Mesh(mesh.devices.reshape(*sizes.values()), tuple(sizes))
    in_specs = (
        P(SEG, None, "y"),
        P(SEG, None, "y"),
        P(SEG, None, "y"),
        P(SEG, None, "y"),
        P(SEG),
        P("y"),
    )
    out_specs = (P(SEG, "y"), P(SEG, "y"), P(SEG))

    def body(*args):
        return on_device(sizes, *args)

    return jax.shard_map(
        body, mesh=torus, in_specs=in_specs, out_specs=out_specs, check_vma=False
    )
```
